256 devices in a mesh: prow: 8 (over z), pcol: 32 (over y, x, core).
Axes of the slice: x: 4, y: 4, z: 8, core: 2. Of those that a mesh axis runs over, the one named last changes fastest.
Arguments:
- points: float32 [1, 32, 2, 1024], P(None, 'pcol'), may hold values from 0 to 1
- range_length: float32 [1], replicated, may hold values from 0.05 to 0.15
- smoothness: int32 [1], replicated, may hold values from 0 to 2
- sketch_bank: bfloat16 [32, 48, 1024], P('pcol'), may hold values from -6 to 6
- sketch_ids: int32 [4, 8, 1, 32], P(None, 'prow', None, 'pcol'), may hold values from 0 to 31
- tile_ranks: int32 [4, 8, 1, 32], P(None, 'prow', None, 'pcol'), may hold values from 16 to 48
Outputs:
- y_factors: float32 [4, 8, 1, 32, 48, 1024], P(None, 'prow', None, 'pcol')
- c_factors: float32 [4, 8, 1, 32, 48, 1024], P(None, 'prow', None, 'pcol')
- tile_error: float32 [4, 8, 1, 32], P(None, 'prow', None, 'pcol')
- rank_total: int32 [1], replicated
The draws below stay inside these ranges and needn't reach their ends.
All inputs are finite; a program needn't handle non-finite values.
Results may differ from the reference program's by a relative error of at most 0.0098.
The reference program's roundings to bfloat16 on the way count: a program that leaves them out, or rounds other values in their place, can miss the bound.
Values may be sent and summed in bfloat16 or wider, within the bound.
A program may use at most 64 MiB of HBM per device.

```python
import math
import jax
import jax.numpy as jnp
import numpy as np
from jax import lax

NB = 1024
RMAX = 48
RMIN = 16
MTB = 1
MT = 32
TRD = 4
SB = 32
N_PROW = 8
N_PCOL = 32


def draw_points(key, part):
    total_bits = max(1, (MT - 1).bit_length())
    x_bits = (total_bits + 1) // 2
    y_bits = total_bits // 2
    blocks = jnp.arange(MT, dtype=jnp.int32)
    cell_x = jnp.zeros((MT,), jnp.float32)
    cell_y = jnp.zeros((MT,), jnp.float32)
    for level in range(total_bits):
        digit = (blocks // 2 ** level % 2).astype(jnp.float32)
        if level % 2 == 0:
            cell_x = cell_x + digit * float(2 ** (level // 2))
        else:
            cell_y = cell_y + digit * float(2 ** (level // 2))
    key_jitter = jax.random.fold_in(key, 11)
    key_spread = jax.random.fold_in(key, 23)
    key_select = jax.random.fold_in(key, 37)
    jitter = jax.random.uniform(key_jitter, (MT, 2, NB), jnp.float32)
    spread = jax.random.uniform(key_spread, (MT, 2, NB), jnp.float32)
    select = jax.random.uniform(key_select, (MT, 1, NB), jnp.float32)
    share = 0.25
    coord_x = (cell_x[:, None] + jitter[:, 0]) / float(2 ** x_bits)
    coord_y = (cell_y[:, None] + jitter[:, 1]) / float(2 ** y_bits)
    local = jnp.stack([coord_x, coord_y], axis=1)
    placed = jnp.where(select < share, spread, local)
    return placed.reshape(MTB, N_PCOL, 2, NB)


def plant(drawn, key, low, largest):
    longest = drawn.shape.index(max(drawn.shape))
    spots = []
    for shift in (0, 1):
        where = [jax.random.randint(jax.random.fold_in(key, axis), (), 0, length) for axis, length in enumerate(drawn.shape)]
        where[longest] = (where[longest] + shift) % drawn.shape[longest]
        spots.append(tuple(where))
    return drawn.at[spots[0]].set(low).at[spots[1]].set(largest)


def block_levels(stream_key, extent, shards, least, high):
    def one(axis_at, parts):
        heights = jax.random.uniform(jax.random.fold_in(jax.random.fold_in(stream_key, 6), axis_at), (parts,), jnp.float32, least / len(shards), high / len(shards))
        return jnp.repeat(jnp.exp(heights), extent[axis_at] // parts).reshape((-1,) + (1,) * (len(extent) - axis_at - 1))

    gain = one(*shards[0])
    for cut in shards[1:]:
        gain = gain * one(*cut)
    return gain


def noise(rng, shape, scale, reach, cuts=(), held_as=jnp.bfloat16):
    entries = scale * jax.random.normal(rng, shape, jnp.float32)
    if cuts:
        entries = entries * block_levels(rng, shape, cuts, -0.22, 0.18)
    return jnp.clip(entries, -reach, reach).astype(held_as)


def setup_inputs(seed: int = 0) -> dict:
    key_list = jax.random.split(jax.random.key(seed), 7)
    points = draw_points(jax.random.fold_in(key_list[6], 71), 0)
    range_length = jnp.clip(jnp.exp(jax.random.uniform(key_list[1], (1,), jnp.float32, math.log(0.05), math.log(0.15))), 0.05, 0.15)
    smoothness = jax.random.randint(key_list[2], (1,), 0, 3).astype(jnp.int32)
    sketch_bank = noise(key_list[3], (SB, RMAX, NB), 1.0, 6.0, ((0, 32),))
    sketch_ids = plant(jax.random.randint(key_list[4], (TRD, N_PROW, MTB, N_PCOL), 0, SB), jax.random.fold_in(key_list[4], 1), 0, SB - 1).astype(jnp.int32)
    tile_ranks = plant(jax.random.randint(key_list[5], (TRD, N_PROW, MTB, N_PCOL), RMIN, RMAX + 1), jax.random.fold_in(key_list[5], 1), RMIN, RMAX).astype(jnp.int32)
    return dict(points=points, range_length=range_length, smoothness=smoothness, sketch_bank=sketch_bank, sketch_ids=sketch_ids, tile_ranks=tile_ranks)


def kernel_factors(smoothness, range_length):
    morton_value = smoothness[0].astype(jnp.float32)
    kernel_scale = jnp.sqrt(2.0 * morton_value + 1.0) / range_length[0]
    linear_factor = jnp.where(smoothness[0] >= 1, 1.0, 0.0).astype(jnp.float32)
    squared_distance = jnp.where(smoothness[0] >= 2, 1.0 / 3.0, 0.0).astype(jnp.float32)
    return (kernel_scale, linear_factor, squared_distance)

def covariance_tile(row_locations, column_locations, kernel_scale, linear_factor, squared_distance):
    offset_horizontal = row_locations[0][:, None] - column_locations[0][None, :]
    offset_vertical = row_locations[1][:, None] - column_locations[1][None, :]
    scaled_distance = kernel_scale * jnp.sqrt(offset_horizontal * offset_horizontal + offset_vertical * offset_vertical)
    return (1.0 + linear_factor * scaled_distance + squared_distance * scaled_distance * scaled_distance) * jnp.exp(-scaled_distance)

def compress(tile_low, sketch, rank):
    keep = jnp.arange(sketch.shape[0]) < rank
    sketch = jnp.where(keep[:, None], sketch, jnp.zeros_like(sketch))
    sketched = lax.dot_general(sketch.astype(jnp.float32), tile_low.astype(jnp.float32), (((1,), (1,)), ((), ())), preferred_element_type=jnp.float32)
    product = jnp.dot(sketched.astype(jnp.bfloat16).astype(jnp.float32), tile_low.astype(jnp.float32), preferred_element_type=jnp.float32)
    gram = jnp.dot(sketched, sketched.T, precision=lax.Precision.HIGHEST)
    shift = 0.1 * jnp.trace(gram) / rank.astype(jnp.float32)
    gram = gram + jnp.diag(jnp.where(keep, shift, jnp.ones_like(shift)))
    factor = jnp.linalg.cholesky(gram)
    coeffs = jax.scipy.linalg.cho_solve((factor, True), product)
    approx = lax.dot_general(sketched, coeffs, (((0,), (0,)), ((), ())), precision=lax.Precision.HIGHEST)
    error = tile_low.astype(jnp.float32) - approx
    return (sketched, coeffs, jnp.sum(error * error))

def reference(points, range_length, smoothness, sketch_bank, sketch_ids, tile_ranks):
    every_block = points.reshape(MT, 2, NB)
    kernel_scale, linear_factor, squared_distance = kernel_factors(smoothness, range_length)
    pairs = np.array([(row, col) for row in range(MT) for col in range(row + 1)], np.int32)
    row_index = jnp.asarray(pairs[:, 0]).astype(jnp.int32)
    col_index = jnp.asarray(pairs[:, 1]).astype(jnp.int32)
    row_major = row_index // N_PROW
    row_minor = row_index % N_PROW
    col_major = col_index // N_PCOL
    col_minor = col_index % N_PCOL
    chosen_ids = sketch_ids[row_major, row_minor, col_major, col_minor]
    chosen_ranks = tile_ranks[row_major, row_minor, col_major, col_minor]

    def one_tile(inputs):
        row_number, column_number, sketch_id, rank = inputs
        tile_block = covariance_tile(every_block[row_number], every_block[column_number], kernel_scale, linear_factor, squared_distance)
        norm_sq = jnp.sum(tile_block * tile_block)
        tile_low = tile_block.astype(jnp.bfloat16)
        sketched, coeffs, err_sq = compress(tile_low, sketch_bank[sketch_id], rank)
        return (sketched, coeffs, norm_sq, err_sq)
    sketched_all, coeffs_all, norm_all, err_all = lax.map(one_tile, (row_index, col_index, chosen_ids, chosen_ranks))
    offdiag = row_index > col_index
    total = jnp.sum(jnp.where(offdiag, 2.0, 1.0) * norm_all)
    errors = jnp.where(offdiag, jnp.sqrt(err_all), jnp.sqrt(norm_all)) * MT / jnp.sqrt(total)
    shape_out = (TRD, N_PROW, MTB, N_PCOL, RMAX, NB)
    y_out = jnp.zeros(shape_out, jnp.float32).at[row_major, row_minor, col_major, col_minor].set(jnp.where(offdiag[:, None, None], sketched_all, 0.0))
    c_out = jnp.zeros(shape_out, jnp.float32).at[row_major, row_minor, col_major, col_minor].set(jnp.where(offdiag[:, None, None], coeffs_all, 0.0))
    err_out = jnp.zeros((TRD, N_PROW, MTB, N_PCOL), jnp.float32).at[row_major, row_minor, col_major, col_minor].set(errors)
    rank_out = jnp.sum(jnp.where(offdiag, chosen_ranks, 0)).astype(jnp.int32).reshape(1)
    return (y_out, c_out, err_out, rank_out)
```

```python
import functools
import math

import jax
import jax.numpy as jnp
from jax import lax
from jax.experimental import pallas as pl
from jax.experimental.pallas import tpu as pltpu
from jax.sharding import PartitionSpec as P

MESH = pl.DeviceIdType.MESH
LOG2E = math.log2(math.e)
F32 = jnp.float32
BF16 = jnp.bfloat16
LANES = 128
ROWS = 32
NT = (((1,), (1,)), ((), ()))
TN = (((0,), (0,)), ((), ()))


def kernel(dims, pts, sketch, reach, smooth, ids, ranks, y_out, c_out, err_out, rank_out,
           rows, bank, low, row_x, row_y, col_x, col_y, prod, inv, norms, sums_z, sums_p, message,
           pts_send, pts_recv, own_sem, first_send, first_recv, second_send, second_recv,
           half_send, half_recv, mirror_send, mirror_recv, z_send, z_recv, p_send, p_recv):
    slots, n_row, n_col, nb, rmax = dims
    p = lax.axis_index("prow")
    q = lax.axis_index("pcol")
    y, x, core = q // 8, lax.rem(q // 2, 4), lax.rem(q, 2)
    partner = q + 1 - 2 * core
    half = nb // 2

    def place(e, f):
        dy = core * e + (1 - core) * f
        dx = (1 - core) * e + core * f
        return lax.rem(y + dy + 8, 4) * 8 + lax.rem(x + dx + 8, 4) * 2 + core

    barrier = pltpu.get_barrier_semaphore()
    for d in range(1, n_col):
        pl.semaphore_signal(barrier, inc=1, device_id={"pcol": lax.rem(q + d, n_col)}, device_id_type=MESH)
    for d in range(1, n_row):
        pl.semaphore_signal(barrier, inc=1, device_id={"prow": lax.rem(p + d, n_row)}, device_id_type=MESH)
    pl.semaphore_wait(barrier, n_col - 1 + n_row - 1)

    is_source = lax.rem(q, n_row) == p
    own_slot = q // n_row

    def point_copy(d):
        return pltpu.make_async_remote_copy(
            pts, rows.at[own_slot], pts_send.at[d], pts_recv.at[own_slot],
            device_id={"pcol": q - d}, device_id_type=MESH)

    for d in range(1, n_col):
        @pl.when(is_source & (q >= d))
        def _():
            point_copy(d).start()

    own_copies = [pltpu.make_async_copy(sketch, bank.at[q], own_sem.at[0])]
    own_copies[0].start()

    def remote(src, dst, send, recv, target):
        return pltpu.make_async_remote_copy(src, dst, send, recv, device_id={"pcol": target}, device_id_type=MESH)

    def first_copy(s):
        return remote(sketch, bank.at[q], first_send.at[s], first_recv.at[s], place(1 - 2 * s, 0))

    def second_copy(e, s):
        block = place(-e, 0)
        src = sketch if e == 0 else bank.at[block]
        return remote(src, bank.at[block], second_send.at[e, s], second_recv.at[e, s], place(0, 1 - 2 * s))

    def half_copy(e, s):
        cols = pl.ds(s * half, half)
        step = 1 - 2 * s
        if e == 4:
            block, target = place(-step, 0), place(step, 0)
        else:
            block, target = place(-e, -step), place(0, step)
        return remote(bank.at[block, :, cols], bank.at[block, :, cols], half_send.at[e, s], half_recv.at[e, s], target)

    def mirror_copy(e, f):
        block = place(-e, -f)
        src = sketch if e == 0 and f == 0 else bank.at[block]
        return remote(src, bank.at[block], mirror_send.at[e, f], mirror_recv.at[e, f], partner)

    def first_recv_wait(s):
        first_copy(s).wait_recv()

    def step0():
        for s in range(2):
            first_copy(s).start()
            second_copy(0, s).start()
        mirror_copy(0, 0).start()

    def step1():
        for s, e in ((0, 1), (1, 3)):
            first_copy(s).wait_recv()
            half_copy(4, s).start()
            for t in range(2):
                second_copy(e, t).start()
            mirror_copy(e, 0).start()

    def step2():
        for s, f in ((0, 1), (1, 3)):
            second_copy(0, s).wait_recv()
            half_copy(0, s).start()
            mirror_copy(0, f).start()
        for s in range(2):
            half_copy(4, s).wait_recv()
        for t in range(2):
            second_copy(2, t).start()
        mirror_copy(2, 0).start()

    def step_second(e):
        for s, f in ((0, 1), (1, 3)):
            second_copy(e, s).wait_recv()
            half_copy(e, s).start()
            mirror_copy(e, f).start()

    def step_tail(e):
        for s in range(2):
            half_copy(e, s).wait_recv()
        mirror_copy(e, 2).start()

    step0()

    s_val = smooth[0]
    root = jnp.where(s_val >= 2, math.sqrt(5.0), jnp.where(s_val >= 1, math.sqrt(3.0), 1.0)).astype(F32)
    scale = (root * LOG2E) / jnp.full((8, LANES), reach[0], F32)
    linear = jnp.where(s_val >= 1, 1.0 / LOG2E, 0.0).astype(F32)
    square = jnp.where(s_val >= 2, 1.0 / (3.0 * LOG2E * LOG2E), 0.0).astype(F32)

    for cb in range(nb // LANES):
        cols = pl.ds(cb * LANES, LANES)
        col_x[:, cols] = jnp.broadcast_to(pts[0:1, cols], (8, LANES)) * scale
        col_y[:, cols] = jnp.broadcast_to(pts[1:2, cols], (8, LANES)) * scale

    norms[...] = jnp.zeros_like(norms)
    for a in range(slots):
        eye = (lax.broadcasted_iota(jnp.int32, (rmax, rmax), 0) == lax.broadcasted_iota(jnp.int32, (rmax, rmax), 1))
        inv[a] = jnp.where(eye, 1.0, 0.0).astype(F32)

    def prepare(a, source):
        for cb in range(nb // LANES):
            cols = pl.ds(cb * LANES, LANES)
            for c, out in ((0, row_x), (1, row_y)):
                line = source[c:c + 1, cols] * scale[0:1, :]
                out[cols, :] = jnp.broadcast_to(line, (LANES, LANES)).T

    def generate(a, part, parts):
        count = nb // ROWS // parts

        def body(g, acc):
            r0 = pl.multiple_of(g * ROWS, ROWS)
            acc = list(acc)
            for rg in range(ROWS // 16):
                r = pl.multiple_of(r0 + rg * 16, 16)
                rx = row_x[pl.ds(r, 16), :]
                ry = row_y[pl.ds(r, 16), :]
                for cb in range(nb // LANES):
                    cols = pl.ds(cb * LANES, LANES)
                    cx, cy = col_x[:, cols], col_y[:, cols]
                    tiles = []
                    for h in range(2):
                        dx = rx[h * 8:h * 8 + 8] - cx
                        dy = ry[h * 8:h * 8 + 8] - cy
                        d2 = jnp.maximum(dx * dx + dy * dy, 1e-30)
                        t = d2 * lax.rsqrt(d2)
                        value = (1.0 + linear * t + square * d2) * jnp.exp2(-t)
                        acc[h] = acc[h] + value * value
                        tiles.append(value)
                    low[a, pl.ds(r, 16), cols] = jnp.concatenate(tiles, 0).astype(BF16)
            return tuple(acc)

        zero = jnp.zeros((8, LANES), F32)
        acc = lax.fori_loop(part * count, (part + 1) * count, body, (zero, zero))
        norms[a] = norms[a] + (acc[0] + acc[1])

    own_points = own_slot
    def tile_part(a, part, parts):
        row = n_row * a + p

        @pl.when(q <= row)
        def _():
            if part == 0:
                @pl.when(q < row)
                def _():
                    remote(pts, rows.at[a], pts_send.at[0], pts_recv.at[a], partner).wait_recv()
                    prepare(a, rows.at[a])

                @pl.when(q == row)
                def _():
                    prepare(a, pts)
            generate(a, part, parts)

    tile_part(3, 0, 2)
    step1()
    tile_part(3, 1, 2)
    step2()
    tile_part(2, 0, 2)
    step_second(1)
    tile_part(2, 1, 2)
    step_second(3)
    tile_part(1, 0, 2)
    step_tail(0)
    step_second(2)
    tile_part(1, 1, 2)
    step_tail(1)
    tile_part(0, 0, 2)
    step_tail(3)
    tile_part(0, 1, 2)
    step_tail(2)

    share = jnp.zeros((8, LANES), F32)
    rank_share = jnp.int32(0)
    for a in range(slots):
        row = n_row * a + p
        weight = jnp.where(q < row, 2.0, jnp.where(q == row, 1.0, 0.0)).astype(F32)
        share = share + weight * norms[a]
        rank_share = rank_share + jnp.where(q < row, ranks[a], 0)
    lane = lax.broadcasted_iota(jnp.int32, (8, LANES), 1)
    sub = lax.broadcasted_iota(jnp.int32, (8, LANES), 0)
    folded = jnp.sum(share, axis=0, keepdims=True)
    sums_z[p] = jnp.where(sub == 0, jnp.broadcast_to(folded, (8, LANES)),
                          jnp.where((sub == 1) & (lane == 0), rank_share.astype(F32), 0.0))

    def z_copy(d):
        return pltpu.make_async_remote_copy(
            sums_z.at[p], sums_z.at[p], z_send.at[d], z_recv.at[d],
            device_id={"prow": lax.rem(p + d, n_row)}, device_id_type=MESH)

    def p_copy(d):
        return pltpu.make_async_remote_copy(
            sums_p.at[q], sums_p.at[q], p_send.at[d], p_recv.at[d],
            device_id={"pcol": lax.rem(q + d, n_col)}, device_id_type=MESH)

    own_copies[0].wait()
    for e in range(4):
        for f in range(4):
            mirror_copy(e, f).wait_recv()

    for d in range(1, n_row):
        z_copy(d).start()

    def products(a):
        row = n_row * a + p

        @pl.when(q < row)
        def _():
            keep = lax.broadcasted_iota(jnp.int32, (rmax, nb), 0) < ranks[a]
            chosen = jnp.where(keep, bank[ids[a]].astype(F32), 0.0).astype(BF16)
            total = jnp.zeros((rmax, nb), F32)
            for mb in range(nb // 256):
                block = low[a, mb * 256:(mb + 1) * 256, :]
                part = lax.dot_general(chosen, block, NT, preferred_element_type=F32)
                y_out[a, :, mb * 256:(mb + 1) * 256] = part
                total = total + jnp.dot(part.astype(BF16), block, preferred_element_type=F32)
            prod[a] = total
            sketched = y_out[a]
            gram = lax.dot_general(sketched, sketched, NT, precision=lax.Precision.HIGHEST, preferred_element_type=F32)
            ri = lax.broadcasted_iota(jnp.int32, (rmax, rmax), 0)
            ci = lax.broadcasted_iota(jnp.int32, (rmax, rmax), 1)
            diag = ri == ci
            trace = jnp.sum(jnp.where(diag, gram, 0.0), keepdims=True)
            shift = 0.1 * trace / jnp.full((1, 1), ranks[a].astype(F32))
            inv[a] = gram + jnp.where(diag, jnp.where(ri < ranks[a], jnp.broadcast_to(shift, (rmax, rmax)), 1.0), 0.0)

    products(3)
    products(2)
    for d in range(1, n_row):
        z_copy(d).wait_recv()
    plane = sums_z[0]
    for d in range(1, n_row):
        plane = plane + sums_z[d]
    sums_p[q] = plane
    products(1)
    products(0)
    for d in range(1, n_col):
        p_copy(d).start()

    ri = lax.broadcasted_iota(jnp.int32, (rmax, rmax), 0)
    ci = lax.broadcasted_iota(jnp.int32, (rmax, rmax), 1)
    mats = [inv[a] for a in range(slots)]
    for k in range(rmax):
        for a in range(slots):
            m = mats[a]
            r = m[k:k + 1, :]
            c = m[:, k:k + 1]
            d = 1.0 / m[k:k + 1, k:k + 1]
            r = jnp.where(ci[0:1] == k, d, r * d)
            m = jnp.where(ci == k, 0.0, m) - c * r
            mats[a] = jnp.where(ri == k, r, m)
    for a in range(slots):
        inv[a] = mats[a]

    def finish(a):
        row = n_row * a + p

        @pl.when(q < row)
        def _():
            coeffs = jnp.dot(inv[a], prod[a], precision=lax.Precision.HIGHEST, preferred_element_type=F32)
            c_out[a] = coeffs
            c_hi = coeffs.astype(BF16)
            c_lo = (coeffs - c_hi.astype(F32)).astype(BF16)
            right = jnp.concatenate([c_hi, c_hi, c_lo], 0)
            acc = jnp.zeros((8, LANES), F32)
            for mb in range(nb // 128):
                part = y_out[a, :, mb * 128:(mb + 1) * 128]
                hi = part.astype(BF16).astype(F32)
                left = jnp.concatenate([hi, part - hi, hi], 0).T.astype(BF16)
                approx = jnp.dot(left, right, preferred_element_type=F32)
                gap = low[a, mb * 128:(mb + 1) * 128, :].astype(F32) - approx
                gap = gap * gap
                for i in range(16):
                    for j in range(nb // LANES):
                        acc = acc + gap[i * 8:i * 8 + 8, j * LANES:(j + 1) * LANES]
            norms[a] = acc

        @pl.when(q >= row)
        def _():
            y_out[a] = jnp.zeros((rmax, nb), F32)
            c_out[a] = jnp.zeros((rmax, nb), F32)

    for a in range(slots):
        finish(a)

    for d in range(1, n_col):
        p_copy(d).wait_recv()
    whole = sums_p[0]
    for d in range(1, n_col):
        whole = whole + sums_p[d]
    total = jnp.sum(whole[0:1, :], keepdims=True)
    ranks_sum = jnp.sum(whole[1:2, :])
    rank_out[0] = ranks_sum.astype(jnp.int32)
    for a in range(slots):
        row = n_row * a + p
        value = jnp.sum(norms[a], keepdims=True)
        value = jnp.sqrt(value) * (n_row * slots) / jnp.sqrt(total)
        value = jnp.where(q <= row, value, 0.0)
        err_out[a] = value[0, 0]

    for d in range(1, n_col):
        @pl.when(is_source & (q >= d))
        def _():
            point_copy(d).wait_send()
        p_copy(d).wait_send()
    for d in range(1, n_row):
        z_copy(d).wait_send()
    for s in range(2):
        first_copy(s).wait_send()
        for e in range(5):
            half_copy(e, s).wait_send()
        for e in range(4):
            second_copy(e, s).wait_send()
    for e in range(4):
        for f in range(4):
            mirror_copy(e, f).wait_send()


def solution(mesh):
    n_row, n_col = mesh.shape["prow"], mesh.shape["pcol"]

    def per_device(points, range_length, smoothness, sketch_bank, sketch_ids, tile_ranks):
        slots = sketch_ids.shape[0]
        nb = points.shape[3]
        rmax = sketch_bank.shape[1]
        dims = (slots, n_row, n_col, nb, rmax)
        vmem = pl.BlockSpec(memory_space=pltpu.VMEM)
        smem = pl.BlockSpec(memory_space=pltpu.SMEM)
        dma = pltpu.SemaphoreType.DMA
        y_out, c_out, err, rank = pl.pallas_call(
            functools.partial(kernel, dims),
            out_shape=(
                jax.ShapeDtypeStruct((slots, rmax, nb), F32),
                jax.ShapeDtypeStruct((slots, rmax, nb), F32),
                jax.ShapeDtypeStruct((slots,), F32),
                jax.ShapeDtypeStruct((1,), jnp.int32),
            ),
            in_specs=[vmem, vmem, smem, smem, smem, smem],
            out_specs=(vmem, vmem, smem, smem),
            scratch_shapes=[
                pltpu.VMEM((slots, 2, nb), F32),
                pltpu.VMEM((n_col, rmax, nb), BF16),
                pltpu.VMEM((slots, nb, nb), BF16),
                pltpu.VMEM((nb, LANES), F32),
                pltpu.VMEM((nb, LANES), F32),
                pltpu.VMEM((8, nb), F32),
                pltpu.VMEM((8, nb), F32),
                pltpu.VMEM((slots, rmax, nb), F32),
                pltpu.VMEM((slots, rmax, rmax), F32),
                pltpu.VMEM((slots, 8, LANES), F32),
                pltpu.VMEM((n_row, 8, LANES), F32),
                pltpu.VMEM((n_col, 8, LANES), F32),
                pltpu.VMEM((8, LANES), F32),
                dma((n_col,)), dma((slots,)), dma((1,)),
                dma((2,)), dma((2,)), dma((4, 2)), dma((4, 2)),
                dma((5, 2)), dma((5, 2)), dma((4, 4)), dma((4, 4)),
                dma((n_row,)), dma((n_row,)), dma((n_col,)), dma((n_col,)),
            ],
            compiler_params=pltpu.CompilerParams(
                collective_id=0, has_side_effects=True, vmem_limit_bytes=60 * 1024 * 1024),
        )(
            points.reshape(2, nb), sketch_bank.reshape(rmax, nb), range_length, smoothness,
            sketch_ids.reshape(slots), tile_ranks.reshape(slots),
        )
        return (
            y_out.reshape(slots, 1, 1, 1, rmax, nb),
            c_out.reshape(slots, 1, 1, 1, rmax, nb),
            err.reshape(slots, 1, 1, 1),
            rank,
        )

    return jax.shard_map(
        per_device,
        mesh=mesh,
        in_specs=(
            P(None, "pcol", None, None),
            P(),
            P(),
            P("pcol", None, None),
            P(None, "prow", None, "pcol"),
            P(None, "prow", None, "pcol"),
        ),
        out_specs=(
            P(None, "prow", None, "pcol", None, None),
            P(None, "prow", None, "pcol", None, None),
            P(None, "prow", None, "pcol"),
            P(),
        ),
        check_vma=False,
    )
```

```python
import functools
import math

import jax
import jax.numpy as jnp
from jax import lax
from jax.experimental import pallas as pl
from jax.experimental.pallas import tpu as pltpu
from jax.sharding import PartitionSpec as P

MESH = pl.DeviceIdType.MESH
LOG2E = math.log2(math.e)
F32 = jnp.float32
BF16 = jnp.bfloat16
LANES = 128
ROWS = 128
VMEM_BYTES = 40 * 1024 * 1024
NT = (((1,), (1,)), ((), ()))


def kernel(dims, pts_in, sketch_in, reach_in, smooth_in, ids_in, ranks_in, y_out, c_out, err_out, rank_out,
           reach, smooth, ids, ranks, pts, rows, far_cols, bank, low, row_x, row_y, col_x, col_y, left, wide, prod, coef, gram_buf, tall, norms, errs,
           zeros, note, far_note, sent_y, sent_c, far_y, far_c, far_err, sums_z, sums_p,
           load_sem, group_send, pts_send, pts_recv, help_send, help_recv, bank_send, bank_recv1, bank_recv2, mirror_recv,
           sum_send, sum_recv, out_sem, zero_sem):
    slots, n_row, n_col, nb, rmax = dims
    p = lax.axis_index("prow")
    q = lax.axis_index("pcol")
    y, x, core = q // 8, lax.rem(q // 2, 4), lax.rem(q, 2)
    partner = q + 1 - 2 * core
    is_home, is_helper = y == 0, y == slots - 1
    pair = lax.rem(q + (slots - 1) * n_row, n_col)
    job_slot = (jnp.where(is_home, 1, slots - 1), 2, y)
    job_on = (q >= 0, y <= 1, q <= n_row * y + p)
    job_off = (q >= 0, y <= 1, q < n_row * y + p)

    def remote(src, dst, send, recv, target):
        return pltpu.make_async_remote_copy(src, dst, send, recv, device_id={"pcol": target}, device_id_type=MESH)

    def all_of(ref, sem):
        pltpu.make_async_copy(ref, ref, sem).wait()

    def place(e, f):
        dy = core * e + (1 - core) * f
        dx = (1 - core) * e + core * f
        return lax.rem(y + dy + 8, 4) * 8 + lax.rem(x + dx + 8, 4) * 2 + core

    loads = [pltpu.make_async_copy(src, dst, load_sem.at[i]) for i, (src, dst) in enumerate((
        (reach_in, reach), (smooth_in, smooth), (ids_in, ids), (ranks_in, ranks), (pts_in, pts),
        (sketch_in, bank.at[q])))]
    barrier = pltpu.get_barrier_semaphore()

    def phase_enter():
        for load in loads:
            load.start()
        for d in range(1, n_col):
            pl.semaphore_signal(barrier, inc=1, device_id={"pcol": lax.rem(q + d, n_col)}, device_id_type=MESH)
        for d in range(1, n_row):
            pl.semaphore_signal(barrier, inc=1, device_id={"prow": lax.rem(p + d, n_row)}, device_id_type=MESH)

    lane = lax.broadcasted_iota(jnp.int32, (8, LANES), 1)
    sub = lax.broadcasted_iota(jnp.int32, (8, LANES), 0)

    zero_copies = [[pltpu.make_async_copy(zeros, out.at[a], zero_sem.at[a]) for a in range(slots)]
                   for out in (y_out, c_out)]

    def phase_setup():
        for load in loads:
            load.wait()
        note[...] = jnp.where(lane == 0, ids[slots - 1], ranks[slots - 1])
        zeros[...] = jnp.zeros((rmax, nb), F32)
        norms[...] = jnp.zeros_like(norms)
        errs[...] = jnp.zeros_like(errs)
        for k in range(3):
            gram_buf[k] = jnp.where(eye, 1.0, 0.0).astype(F32)
        for a in range(slots):
            @pl.when(q >= n_row * a + p)
            def _():
                for i in range(2):
                    zero_copies[i][a].start()

    mat_r = lax.broadcasted_iota(jnp.int32, (rmax, rmax), 0)
    mat_c = lax.broadcasted_iota(jnp.int32, (rmax, rmax), 1)
    eye = mat_r == mat_c

    def phase_barrier():
        pl.semaphore_wait(barrier, n_col - 1 + n_row - 1)

    is_source = lax.rem(q, n_row) == p

    def group_copy(g, i):
        return remote(pts, rows.at[y], group_send.at[g], pts_recv.at[y], g * 8 + i)

    def sends_group(g):
        return is_source & jnp.where(y == slots - 1, (g > 0) & (g < slots - 1), g < y)

    def point_copy(d):
        return remote(pts, rows.at[y], pts_send.at[d], pts_recv.at[y], y * 8 + lax.rem(q + d, 8))

    def sends_points(d):
        return is_source & ((y == slots - 1) | (lax.rem(q, 8) + d >= 8))

    help_copies = (
        lambda: remote(pts, far_cols, help_send.at[0], help_recv.at[0], pair),
        lambda: remote(note, far_note, help_send.at[1], help_recv.at[1], pair),
    )
    back = lax.rem(q + n_row, n_col)
    back_copies = (
        lambda: remote(sent_y, far_y, help_send.at[2], help_recv.at[2], back),
        lambda: remote(sent_c, far_c, help_send.at[3], help_recv.at[3], back),
        lambda: remote(errs.at[0], far_err, help_send.at[4], help_recv.at[4], back),
    )

    def phase_points():
        for g in range(slots - 1):
            @pl.when(sends_group(g))
            def _():
                for i in range(8):
                    group_copy(g, i).start()
        for d in range(1, 8):
            @pl.when(sends_points(d))
            def _():
                point_copy(d).start()

        @pl.when(is_home)
        def _():
            for c in help_copies:
                c().start()

    def first_copy(d):
        return remote(bank.at[q], bank.at[q], bank_send.at[0], bank_recv1.at[d], place(d, 0))

    def second_copy(e, d):
        block = place(-e, 0)
        return remote(bank.at[block], bank.at[block], bank_send.at[0], bank_recv2.at[e], place(0, d))

    def mirror_copy(e, f):
        block = place(-e, -f)
        return remote(bank.at[block], bank.at[block], bank_send.at[0], mirror_recv.at[0], partner)

    def step_own():
        for d in (1, 3, 2):
            first_copy(d).start()
        for d in (1, 3, 2):
            second_copy(0, d).start()
        mirror_copy(0, 0).start()

    def step_first(e):
        first_copy(e).wait_recv()
        for d in (1, 3, 2):
            second_copy(e, d).start()
        mirror_copy(e, 0).start()

    def step_second(e):
        all_of(bank.at[0:3], bank_recv2.at[e])
        for d in (1, 3, 2):
            mirror_copy(e, d).start()

    def prepare_rows(source):
        for cb in range(nb // LANES):
            cols = pl.ds(cb * LANES, LANES)
            for c, out in ((0, row_x), (1, row_y)):
                line = source[c:c + 1, cols] * scale[0:1, :]
                out[cols, :] = jnp.broadcast_to(line, (LANES, LANES)).T

    def prepare_cols(source):
        for cb in range(nb // LANES):
            cols = pl.ds(cb * LANES, LANES)
            col_x[:, cols] = jnp.broadcast_to(source[0:1, cols], (8, LANES)) * scale
            col_y[:, cols] = jnp.broadcast_to(source[1:2, cols], (8, LANES)) * scale

    def generate(k, part, parts):
        count = nb // ROWS // parts

        def body(g, acc):
            r0 = pl.multiple_of(g * ROWS, ROWS)
            acc = list(acc)
            for rg in range(ROWS // 16):
                r = pl.multiple_of(r0 + rg * 16, 16)
                rx = row_x[pl.ds(r, 16), :]
                ry = row_y[pl.ds(r, 16), :]
                for cb in range(nb // LANES):
                    cols = pl.ds(cb * LANES, LANES)
                    cx, cy = col_x[:, cols], col_y[:, cols]
                    tiles = []
                    for h in range(2):
                        dx = rx[h * 8:h * 8 + 8] - cx
                        dy = ry[h * 8:h * 8 + 8] - cy
                        d2 = jnp.maximum(dx * dx + dy * dy, 1e-30)
                        t = d2 * lax.rsqrt(d2)
                        value = (1.0 + linear * t + square * d2) * jnp.exp2(-t)
                        acc[h] = acc[h] + value * value
                        tiles.append(value)
                    low[k, pl.ds(r, 16), cols] = jnp.concatenate(tiles, 0).astype(BF16)
            return tuple(acc)

        zero = jnp.zeros((8, LANES), F32)
        acc = lax.fori_loop(part * count, (part + 1) * count, body, (zero, zero))
        norms[k] = norms[k] + (acc[0] + acc[1])

    def row_block(a):
        @pl.when(q == n_row * a + p)
        def _():
            prepare_rows(pts)

        @pl.when(q != n_row * a + p)
        def _():
            remote(pts, rows.at[a], pts_send.at[0], pts_recv.at[a], partner).wait_recv()
            prepare_rows(rows.at[a])

    def tile_part(k, part):
        @pl.when(job_on[k])
        def _():
            if part == 0 and k == 0:
                @pl.when(is_helper)
                def _():
                    help_copies[0]().wait_recv()
                    help_copies[1]().wait_recv()
                    prepare_cols(far_cols)

                @pl.when(jnp.logical_not(is_helper))
                def _():
                    prepare_cols(pts)
                for a in (1, slots - 1):
                    @pl.when(job_slot[0] == a)
                    def _():
                        row_block(a)
            if part == 0 and k == 1:
                row_block(2)
            if part == 0 and k == 2:
                @pl.when(is_helper)
                def _():
                    prepare_cols(pts)
                for a in range(slots - 1):
                    @pl.when(y == a)
                    def _():
                        row_block(a)
            generate(k, part, 4)

    def z_copy(d):
        return pltpu.make_async_remote_copy(
            sums_z.at[p], sums_z.at[p], sum_send.at[0], sum_recv.at[0],
            device_id={"prow": lax.rem(p + d, n_row)}, device_id_type=MESH)

    def p_copy(d):
        return remote(sums_p.at[q], sums_p.at[q], sum_send.at[1], sum_recv.at[1], lax.rem(q + d, n_col))

    def phase_share():
        share = jnp.zeros((8, LANES), F32)
        for k in range(3):
            weight = jnp.where(job_off[k], 2.0, jnp.where(job_on[k], 1.0, 0.0)).astype(F32)
            share = share + weight * norms[k]
        rank_share = jnp.int32(0)
        for a in range(slots):
            rank_share = rank_share + jnp.where(q < n_row * a + p, ranks[a], 0)
        folded = jnp.sum(share, axis=0, keepdims=True)
        sums_z[p] = jnp.where(sub == 0, jnp.broadcast_to(folded, (8, LANES)),
                              jnp.where((sub == 1) & (lane == 0), rank_share.astype(F32), 0.0))

    def wait_bank():
        all_of(bank.at[0:16], mirror_recv.at[0])

    def send_z():
        for d in range(1, n_row):
            z_copy(d).start()

    def y_copy(k):
        return pltpu.make_async_copy(wide.at[k], y_out.at[job_slot[k]], out_sem.at[0, k])

    def c_copy(k):
        return pltpu.make_async_copy(coef.at[k], c_out.at[job_slot[k]], out_sem.at[1, k])

    def ranks_of(k):
        own = ranks[job_slot[k]]
        return jnp.where(is_helper, far_note[0:1, 1:2][0, 0], own) if k == 0 else own

    def id_of(k):
        own = ids[job_slot[k]]
        return jnp.where(is_helper, far_note[0:1, 0:1][0, 0], own) if k == 0 else own

    def products(k):
        @pl.when(job_off[k])
        def _():
            rank = ranks_of(k)
            keep = lax.broadcasted_iota(jnp.int32, (rmax, nb), 0) < rank
            chosen = jnp.where(keep, bank[id_of(k)].astype(F32), 0.0).astype(BF16)
            triple = jnp.concatenate([chosen, chosen, chosen], 0)
            middle = lax.broadcasted_iota(jnp.int32, (LANES, 3 * rmax), 1)
            middle = (middle >= rmax) & (middle < 2 * rmax)
            tall[...] = lax.dot_general(low[k], triple, NT, preferred_element_type=F32)
            for mb in range(nb // LANES):
                part = tall[mb * LANES:(mb + 1) * LANES, :]
                high = part.astype(BF16).astype(F32)
                left[k, mb * LANES:(mb + 1) * LANES, :] = jnp.where(middle, part - high, high).astype(BF16)
                wide[k, :, mb * LANES:(mb + 1) * LANES] = part[:, :LANES].T[:rmax]
            sketched = wide[k]
            high = sketched.astype(BF16)
            rest = (sketched - high.astype(F32)).astype(BF16)
            if k == 0:
                sent_y[...] = high
            prod[k] = jnp.dot(high, low[k], preferred_element_type=F32)
            both = lax.dot_general(high, jnp.concatenate([high, rest], 0), NT, preferred_element_type=F32)
            cross = both[:, rmax:]
            gram = both[:, :rmax] + (cross + cross.T)
            trace = jnp.sum(jnp.where(eye, gram, 0.0), keepdims=True)
            shift = 0.1 * trace / jnp.full((1, 1), rank.astype(F32))
            gram_buf[k] = gram + jnp.where(
                eye, jnp.where(mat_r < rank, jnp.broadcast_to(shift, (rmax, rmax)), 1.0), 0.0)

    def send_y(k):
        @pl.when(job_off[k])
        def _():
            if k == 0:
                @pl.when(is_helper)
                def _():
                    back_copies[0]().start()

                @pl.when(jnp.logical_not(is_helper))
                def _():
                    y_copy(k).start()
            else:
                y_copy(k).start()

    def invert(jobs):
        mats = [gram_buf[k] for k in jobs]
        b = 8
        row8 = lax.broadcasted_iota(jnp.int32, (b, rmax), 0)
        col8 = lax.broadcasted_iota(jnp.int32, (b, rmax), 1)
        for k0 in range(0, rmax, b):
            spread = [[[jnp.broadcast_to(m[i:i + b, k0 + j:k0 + j + 1], (b, rmax)) for j in range(b)]
                       for i in range(0, rmax, b)] for m in mats]
            for n in range(len(mats)):
                m = mats[n]
                d = list(spread[n][k0 // b])
                for j in range(b):
                    inverse = 1.0 / d[j][j:j + 1, :]
                    for i in range(b):
                        if i != j:
                            f = d[i][j:j + 1, :] * inverse
                            d[i] = jnp.where(row8 == j, f, d[i] - d[j] * f)
                    d[j] = jnp.where(row8 == j, inverse, -(d[j] * inverse))
                panel = m[k0:k0 + b]
                r = d[0] * panel[0:1]
                for j in range(1, b):
                    r = r + d[j] * panel[j:j + 1]
                for j in range(b):
                    r = jnp.where(col8 == k0 + j, d[j], r)
                inside = (col8 >= k0) & (col8 < k0 + b)
                out = []
                for i in range(0, rmax, b):
                    if i == k0:
                        out.append(r)
                        continue
                    piece = jnp.where(inside, 0.0, m[i:i + b])
                    for j in range(b):
                        piece = piece - spread[n][i // b][j] * r[j:j + 1]
                    out.append(piece)
                mats[n] = jnp.concatenate(out, 0)
        return mats

    def finish(k, inverse):
        coeffs = jnp.dot(inverse, prod[k], precision=lax.Precision.HIGHEST, preferred_element_type=F32)
        coef[k] = coeffs
        c_hi = coeffs.astype(BF16)
        c_lo = (coeffs - c_hi.astype(F32)).astype(BF16)
        if k == 0:
            sent_c[...] = c_hi
        right = jnp.concatenate([c_hi, c_hi, c_lo], 0)
        acc = [jnp.zeros((8, LANES), F32) for _ in range(4)]
        width, height = 256, 512
        for nt in range(nb // width):
            for mt in range(nb // height):
                span, cols = slice(mt * height, (mt + 1) * height), slice(nt * width, (nt + 1) * width)
                approx = jnp.dot(left[k, span, :], right[:, cols], preferred_element_type=F32)
                gap = low[k, span, cols].astype(F32) - approx
                for i in range(height // 8):
                    for j in range(width // LANES):
                        piece = gap[i * 8:i * 8 + 8, j * LANES:(j + 1) * LANES]
                        n = (2 * i + j) % 4
                        acc[n] = acc[n] + piece * piece
        errs[k] = (acc[0] + acc[1]) + (acc[2] + acc[3])

    def phase_early():
        @pl.when(is_helper)
        def _():
            finish(0, invert((0,))[0])
            back_copies[1]().start()

    def phase_invert():
        mats = invert((0, 1, 2))
        for k in range(3):
            gram_buf[k] = mats[k]

    def phase_finish(k):
        @pl.when(job_off[k] & jnp.logical_not(is_helper) if k == 0 else job_off[k])
        def _():
            finish(k, gram_buf[k])
            c_copy(k).start()

    def wait_z():
        all_of(sums_z.at[0:n_row - 1], sum_recv.at[0])
        plane = sums_z[0]
        for d in range(1, n_row):
            plane = plane + sums_z[d]
        sums_p[q] = plane

    def send_p():
        for d in range(1, n_col):
            p_copy(d).start()

        @pl.when(is_helper)
        def _():
            back_copies[2]().start()

    def phase_far_y():
        @pl.when(is_home)
        def _():
            back_copies[0]().wait_recv()
            wide[3] = far_y[...].astype(F32)
            pltpu.make_async_copy(wide.at[3], y_out.at[slots - 1], out_sem.at[0, 3]).start()

    def phase_far():
        @pl.when(is_home)
        def _():
            for c in back_copies[1:]:
                c().wait_recv()
            coef[3] = far_c[...].astype(F32)
            pltpu.make_async_copy(coef.at[3], c_out.at[slots - 1], out_sem.at[1, 3]).start()

    def total_error():
        all_of(sums_p.at[0:n_col - 1], sum_recv.at[1])
        whole = sums_p[0]
        for d in range(1, n_col):
            whole = whole + sums_p[d]
        total = jnp.sum(whole[0:1, :], keepdims=True)
        rank_out[0] = jnp.sum(whole[1:2, :]).astype(jnp.int32)
        factor = (n_row * slots) / jnp.sqrt(total)
        values = []
        for k in range(3):
            source = jnp.where(job_off[k], errs[k], norms[k])
            value = jnp.sqrt(jnp.sum(source, keepdims=True)) * factor
            values.append(jnp.where(job_on[k], value, 0.0))
        far = jnp.sqrt(jnp.sum(far_err[...], keepdims=True)) * factor
        for a in range(slots):
            out = jnp.zeros((1, 1), F32)
            for k in range(3):
                mine = (job_slot[k] == a) & job_on[k]
                if k == 0:
                    mine = mine & jnp.logical_not(is_helper)
                out = jnp.where(mine, values[k], out)
            if a == slots - 1:
                out = jnp.where(is_home, far, out)
            err_out[a] = out[0, 0]

    def wait_sends():
        for g in range(slots - 1):
            @pl.when(sends_group(g))
            def _():
                all_of(row_x.at[0:128], group_send.at[g])
        for d in range(1, 8):
            @pl.when(sends_points(d))
            def _():
                point_copy(d).wait_send()
        all_of(sums_p.at[0:n_col - 1], sum_send.at[1])
        all_of(sums_z.at[0:n_row - 1], sum_send.at[0])
        all_of(bank.at[0:31], bank_send.at[0])
        for a in range(slots):
            @pl.when(q >= n_row * a + p)
            def _():
                pltpu.make_async_copy(wide.at[0:2], wide.at[0:2], zero_sem.at[a]).wait()

        @pl.when(is_home)
        def _():
            for c in help_copies:
                c().wait_send()
            pltpu.make_async_copy(wide.at[3], y_out.at[slots - 1], out_sem.at[0, 3]).wait()
            pltpu.make_async_copy(coef.at[3], c_out.at[slots - 1], out_sem.at[1, 3]).wait()

        @pl.when(is_helper)
        def _():
            for c in back_copies:
                c().wait_send()
        for k in range(3):
            @pl.when(job_off[k] & jnp.logical_not(is_helper) if k == 0 else job_off[k])
            def _():
                y_copy(k).wait()
                c_copy(k).wait()

    phase_enter()
    phase_setup()
    s_val = smooth[0]
    root = jnp.where(s_val >= 2, math.sqrt(5.0), jnp.where(s_val >= 1, math.sqrt(3.0), 1.0)).astype(F32)
    scale = (root * LOG2E) / jnp.full((8, LANES), reach[0], F32)
    linear = jnp.where(s_val >= 1, 1.0 / LOG2E, 0.0).astype(F32)
    square = jnp.where(s_val >= 2, 1.0 / (3.0 * LOG2E * LOG2E), 0.0).astype(F32)
    phase_barrier()
    phase_points()
    step_own()
    tile_part(0, 0)
    step_first(1)
    step_first(3)
    tile_part(0, 1)
    tile_part(0, 2)
    step_first(2)
    tile_part(0, 3)
    tile_part(1, 0)
    step_second(0)
    tile_part(1, 1)
    tile_part(1, 2)
    tile_part(1, 3)
    tile_part(2, 0)
    step_second(1)
    tile_part(2, 1)
    step_second(3)
    tile_part(2, 2)
    tile_part(2, 3)
    phase_share()
    step_second(2)
    send_z()
    wait_bank()
    products(0)
    send_y(0)
    phase_early()
    products(1)
    send_y(1)
    products(2)
    send_y(2)
    wait_z()
    phase_invert()
    send_p()
    phase_finish(0)
    phase_finish(1)
    phase_far_y()
    phase_finish(2)
    phase_far()
    total_error()
    wait_sends()


def solution(mesh):
    n_row, n_col = mesh.shape["prow"], mesh.shape["pcol"]

    def per_device(points, range_length, smoothness, sketch_bank, sketch_ids, tile_ranks):
        slots = sketch_ids.shape[0]
        nb = points.shape[3]
        rmax = sketch_bank.shape[1]
        dims = (slots, n_row, n_col, nb, rmax)
        anywhere = pl.BlockSpec(memory_space=pl.ANY)
        vmem = pltpu.VMEM
        hbm = pl.BlockSpec(memory_space=pltpu.HBM)
        scalars = pl.BlockSpec(memory_space=pltpu.SMEM)
        smem = pltpu.SMEM
        dma = pltpu.SemaphoreType.DMA
        y_out, c_out, err, rank = pl.pallas_call(
            functools.partial(kernel, dims),
            out_shape=(
                jax.ShapeDtypeStruct((slots, rmax, nb), F32),
                jax.ShapeDtypeStruct((slots, rmax, nb), F32),
                jax.ShapeDtypeStruct((slots,), F32),
                jax.ShapeDtypeStruct((1,), jnp.int32),
            ),
            in_specs=[hbm] * 6,
            out_specs=(anywhere, anywhere, scalars, scalars),
            scratch_shapes=[
                smem((1,), F32), smem((1,), jnp.int32), smem((slots,), jnp.int32), smem((slots,), jnp.int32),
                vmem((2, nb), F32), vmem((slots, 2, nb), F32), vmem((2, nb), F32),
                vmem((n_col, rmax, nb), BF16), vmem((3, nb, nb), BF16),
                vmem((nb, LANES), F32), vmem((nb, LANES), F32), vmem((8, nb), F32), vmem((8, nb), F32),
                vmem((3, nb, 3 * rmax), BF16), vmem((4, rmax, nb), F32), vmem((3, rmax, nb), F32),
                vmem((4, rmax, nb), F32), vmem((3, rmax, rmax), F32), vmem((nb, 3 * rmax), F32),
                vmem((3, 8, LANES), F32), vmem((3, 8, LANES), F32),
                vmem((rmax, nb), F32), vmem((8, LANES), jnp.int32), vmem((8, LANES), jnp.int32),
                vmem((rmax, nb), BF16), vmem((rmax, nb), BF16), vmem((rmax, nb), BF16), vmem((rmax, nb), BF16),
                vmem((8, LANES), F32), vmem((n_row, 8, LANES), F32), vmem((n_col, 8, LANES), F32),
                dma((6,)), dma((3,)), dma((8,)), dma((slots,)), dma((5,)), dma((5,)),
                dma((1,)), dma((4,)), dma((4,)), dma((1,)), dma((2,)), dma((2,)), dma((2, 4)), dma((slots,)),
            ],
            compiler_params=pltpu.CompilerParams(
                collective_id=0, has_side_effects=True, vmem_limit_bytes=VMEM_BYTES),
        )(
            points.reshape(2, nb), sketch_bank.reshape(rmax, nb), range_length, smoothness,
            sketch_ids.reshape(slots), tile_ranks.reshape(slots),
        )
        return (
            y_out.reshape(slots, 1, 1, 1, rmax, nb),
            c_out.reshape(slots, 1, 1, 1, rmax, nb),
            err.reshape(slots, 1, 1, 1),
            rank,
        )

    return jax.shard_map(
        per_device,
        mesh=mesh,
        in_specs=(
            P(None, "pcol", None, None),
            P(),
            P(),
            P("pcol", None, None),
            P(None, "prow", None, "pcol"),
            P(None, "prow", None, "pcol"),
        ),
        out_specs=(
            P(None, "prow", None, "pcol", None, None),
            P(None, "prow", None, "pcol", None, None),
            P(None, "prow", None, "pcol"),
            P(),
        ),
        check_vma=False,
    )
```

```python
import functools
import math

import jax
import jax.numpy as jnp
from jax import lax
from jax.experimental import pallas as pl
from jax.experimental.pallas import tpu as pltpu
from jax.sharding import PartitionSpec as P

MESH = pl.DeviceIdType.MESH
LOG2E = math.log2(math.e)
F32 = jnp.float32
BF16 = jnp.bfloat16
LANES = 128
VMEM_BYTES = 40 * 1024 * 1024
NT = (((1,), (1,)), ((), ()))


def kernel(dims, pts_in, sketch_in, ids_in, ranks_in, reach_in, smooth_in, y_out, c_out, err_out, rank_out,
           reach, smooth, ids, ranks, pts, rows, far_cols, bank, low, row_buf, col_x, col_y, left, wide, prod, coef, full, norms, errs,
           note, far_note, sent_y, sent_c, far_y, far_c, far_err, sums_z, sums_p,
           load_sem, group_send, pts_send, pts_recv, help_send, help_recv, bank_send, bank_recv1, bank_recv2, half_recv, mirror_recv,
           sum_send, sum_recv, out_sem):
    slots, n_row, n_col, nb, rmax = dims
    p = lax.axis_index("prow")
    q = lax.axis_index("pcol")
    y, x, core = q // 8, lax.rem(q // 2, 4), lax.rem(q, 2)
    partner = q + 1 - 2 * core
    is_home, is_helper = y == 0, y == slots - 1
    pair = lax.rem(q + (slots - 1) * n_row, n_col)
    job_slot = (jnp.where(is_home, 1, slots - 1), jnp.where(y == 2, 1, 2), y)
    job_on = (q >= 0, y <= 1, q <= n_row * y + p)
    job_off = (q >= 0, y <= 1, q < n_row * y + p)

    def remote(src, dst, send, recv, target):
        return pltpu.make_async_remote_copy(src, dst, send, recv, device_id={"pcol": target}, device_id_type=MESH)

    def all_of(ref, sem):
        pltpu.make_async_copy(ref, ref, sem).wait()

    def place(e, f):
        dy = core * e + (1 - core) * f
        dx = (1 - core) * e + core * f
        return lax.rem(y + dy + 8, 4) * 8 + lax.rem(x + dx + 8, 4) * 2 + core

    loads = [pltpu.make_async_copy(src, dst, load_sem.at[i]) for i, (src, dst) in enumerate((
        (ids_in, ids), (ranks_in, ranks), (smooth_in, smooth), (reach_in, reach), (pts_in, pts),
        (sketch_in, bank.at[q])))]
    barrier = pltpu.get_barrier_semaphore()

    def phase_enter():
        for load in loads:
            load.start()
        for d in range(1, n_col):
            pl.semaphore_signal(barrier, inc=1, device_id={"pcol": lax.rem(q + d, n_col)}, device_id_type=MESH)
        for d in range(1, n_row):
            pl.semaphore_signal(barrier, inc=1, device_id={"prow": lax.rem(p + d, n_row)}, device_id_type=MESH)

    lane = lax.broadcasted_iota(jnp.int32, (8, LANES), 1)
    sub = lax.broadcasted_iota(jnp.int32, (8, LANES), 0)

    def phase_setup():
        for load in loads:
            load.wait()
        note[...] = jnp.where(lane == 0, ids[slots - 1], ranks[slots - 1])
        wide[...] = jnp.zeros_like(wide)
        coef[...] = jnp.zeros_like(coef)
        norms[...] = jnp.zeros_like(norms)
        errs[...] = jnp.zeros_like(errs)

    mat_r = lax.broadcasted_iota(jnp.int32, (rmax, rmax), 0)
    mat_c = lax.broadcasted_iota(jnp.int32, (rmax, rmax), 1)
    eye = mat_r == mat_c

    def phase_barrier():
        pl.semaphore_wait(barrier, n_col - 1 + n_row - 1)

    is_source = lax.rem(q, n_row) == p

    def group_copy(g, i):
        return remote(pts, rows.at[y], group_send.at[g], pts_recv.at[y], g * 8 + i)

    def sends_group(g):
        return is_source & jnp.where(y == slots - 1, (g > 0) & (g < slots - 1), g < y)

    def point_copy(d):
        return remote(pts, rows.at[y], pts_send.at[d], pts_recv.at[y], y * 8 + lax.rem(q + d, 8))

    def sends_points(d):
        return is_source & ((y == slots - 1) | (lax.rem(q, 8) + d >= 8))

    help_copies = (
        lambda: remote(pts, far_cols, help_send.at[0], help_recv.at[0], pair),
        lambda: remote(note, far_note, help_send.at[1], help_recv.at[1], pair),
    )
    back = lax.rem(q + n_row, n_col)
    back_copies = (
        lambda: remote(sent_y, far_y, help_send.at[2], help_recv.at[2], back),
        lambda: remote(sent_c, far_c, help_send.at[3], help_recv.at[3], back),
        lambda: remote(errs.at[0], far_err, help_send.at[4], help_recv.at[4], back),
    )

    def phase_points():
        for g in range(slots - 1):
            @pl.when(sends_group(g))
            def _():
                for i in range(8):
                    group_copy(g, i).start()
        for d in range(1, 8):
            @pl.when(sends_points(d))
            def _():
                point_copy(d).start()

        @pl.when(is_home)
        def _():
            for c in help_copies:
                c().start()

    def first_copy(d):
        return remote(bank.at[q], bank.at[q], bank_send.at[0], bank_recv1.at[d], place(d, 0))

    def second_copy(e, d):
        block = place(-e, 0)
        return remote(bank.at[block], bank.at[block], bank_send.at[0], bank_recv2.at[e], place(0, d))

    def half_copy(e, d):
        block = place(-e, -d)
        cols = pl.ds(0 if d == 1 else nb // 2, nb // 2)
        return remote(bank.at[block, :, cols], bank.at[block, :, cols], bank_send.at[0], half_recv.at[e], place(0, d))

    def mirror_copy(e, f):
        block = place(-e, -f)
        return remote(bank.at[block], bank.at[block], bank_send.at[0], mirror_recv.at[0], partner)

    def ways(e):
        return (1, 3, 2) if e == 2 else (1, 3)

    def step_own():
        for d in (1, 3, 2):
            first_copy(d).start()
        for d in ways(0):
            second_copy(0, d).start()
        mirror_copy(0, 0).start()

    def step_first(e):
        first_copy(e).wait_recv()
        for d in ways(e):
            second_copy(e, d).start()
        mirror_copy(e, 0).start()

    def step_second(e):
        all_of(bank.at[0:len(ways(e))], bank_recv2.at[e])
        if e != 2:
            for d in (1, 3):
                half_copy(e, d).start()
        for d in ways(e):
            mirror_copy(e, d).start()

    def step_half(e):
        all_of(bank.at[0:1], half_recv.at[e])
        mirror_copy(e, 2).start()

    def prepare_rows(k, source):
        for cb in range(nb // LANES):
            cols = pl.ds(cb * LANES, LANES)
            for c in range(2):
                row_buf[k, c, cols, :] = jnp.broadcast_to(source[c:c + 1, cols] * scale[0:1, :], (LANES, LANES)).T

    def prepare_cols(source):
        for cb in range(nb // LANES):
            cols = pl.ds(cb * LANES, LANES)
            col_x[:, cols] = jnp.broadcast_to(source[0:1, cols], (8, LANES)) * scale
            col_y[:, cols] = jnp.broadcast_to(source[1:2, cols], (8, LANES)) * scale

    def generate(k, buf, g):
        acc = [jnp.zeros((8, LANES), F32) for _ in range(2)]
        for rg in range(LANES // 16):
            r = pl.multiple_of(g * LANES + rg * 16, 16)
            rx = row_buf[buf, 0, pl.ds(r, 16), :]
            ry = row_buf[buf, 1, pl.ds(r, 16), :]
            for cb in range(nb // LANES):
                cols = pl.ds(cb * LANES, LANES)
                cx, cy = col_x[:, cols], col_y[:, cols]
                tiles = []
                for h in range(2):
                    dx = rx[h * 8:h * 8 + 8] - cx
                    dy = ry[h * 8:h * 8 + 8] - cy
                    d2 = jnp.maximum(dx * dx + dy * dy, 1e-30)
                    t = d2 * lax.rsqrt(d2)
                    value = (1.0 + linear * t + square * d2) * jnp.exp2(-t)
                    acc[h] = acc[h] + value * value
                    tiles.append(value)
                low[k, pl.ds(r, 16), cols] = jnp.concatenate(tiles, 0).astype(BF16)
        norms[k] = norms[k] + (acc[0] + acc[1])

    def row_block(k, a):
        @pl.when(q == n_row * a + p)
        def _():
            prepare_rows(k, pts)

        @pl.when(q != n_row * a + p)
        def _():
            remote(pts, rows.at[a], pts_send.at[0], pts_recv.at[a], partner).wait_recv()
            prepare_rows(k, rows.at[a])

    job_rows = (0, 1, jnp.where(is_helper, 0, 2))

    def phase_rows(k):
        if k == 0:
            @pl.when(is_helper)
            def _():
                help_copies[0]().wait_recv()
                help_copies[1]().wait_recv()
                prepare_cols(far_cols)

            @pl.when(jnp.logical_not(is_helper))
            def _():
                prepare_cols(pts)
            for a in (1, slots - 1):
                @pl.when(job_slot[0] == a)
                def _():
                    row_block(0, a)
        if k == 1:
            @pl.when(job_on[1])
            def _():
                row_block(1, 2)
        if k == 2:
            for a in range(slots - 1):
                @pl.when((y == a) & job_on[2])
                def _():
                    row_block(2, a)

    def phase_cols():
        @pl.when(is_helper)
        def _():
            prepare_cols(pts)

    def tile(k, first, last):
        @pl.when(job_on[k])
        def _():
            def body(g, carry):
                generate(k, job_rows[k], g)
                return carry

            lax.fori_loop(first, last, body, 0)

    def z_copy(d):
        return pltpu.make_async_remote_copy(
            sums_z.at[p], sums_z.at[p], sum_send.at[0], sum_recv.at[0],
            device_id={"prow": lax.rem(p + d, n_row)}, device_id_type=MESH)

    def p_copy(d):
        return remote(sums_p.at[q], sums_p.at[q], sum_send.at[1], sum_recv.at[1], lax.rem(q + d, n_col))

    def phase_share():
        share = jnp.zeros((8, LANES), F32)
        for k in range(3):
            weight = jnp.where(job_off[k], 2.0, jnp.where(job_on[k], 1.0, 0.0)).astype(F32)
            share = share + weight * norms[k]
        rank_share = jnp.int32(0)
        for a in range(slots):
            rank_share = rank_share + jnp.where(q < n_row * a + p, ranks[a], 0)
        folded = jnp.sum(share, axis=0, keepdims=True)
        sums_z[p] = jnp.where(sub == 0, jnp.broadcast_to(folded, (8, LANES)),
                              jnp.where((sub == 1) & (lane == 0), rank_share.astype(F32), 0.0))

    def wait_bank():
        all_of(bank.at[0:16], mirror_recv.at[0])

    def send_z():
        for d in range(1, n_row):
            z_copy(d).start()

    y_copy = pltpu.make_async_copy(wide, y_out, out_sem.at[0])
    c_copy = pltpu.make_async_copy(coef, c_out, out_sem.at[1])

    def ranks_of(k):
        own = ranks[job_slot[k]]
        return jnp.where(is_helper, far_note[0:1, 1:2][0, 0], own) if k == 0 else own

    def id_of(k):
        own = ids[job_slot[k]]
        return jnp.where(is_helper, far_note[0:1, 0:1][0, 0], own) if k == 0 else own

    def project(k):
        rank = ranks_of(k)
        keep = lax.broadcasted_iota(jnp.int32, (rmax, nb), 0) < rank
        chosen = jnp.where(keep, bank[id_of(k)].astype(F32), 0.0).astype(BF16)
        sketched = lax.dot_general(chosen, low[k], NT, preferred_element_type=F32)
        high = sketched.astype(BF16)
        rest = sketched - high.astype(F32)
        middle = rest.astype(BF16)
        left[k] = jnp.concatenate([high, middle, (rest - middle.astype(F32)).astype(BF16)], 0)
        wide[job_slot[k]] = jnp.where(job_off[k], sketched, 0.0)

    def squares(k):
        @pl.when(job_off[k])
        def _():
            acc = [jnp.zeros((16, LANES), F32) for _ in range(4)]
            for r in range(0, nb, 16):
                for cb in range(nb // LANES):
                    value = low[k, r:r + 16, cb * LANES:(cb + 1) * LANES].astype(F32)
                    acc[cb % 4] = acc[cb % 4] + value * value
            acc = (acc[0] + acc[1]) + (acc[2] + acc[3])
            errs[k] = acc[:8] + acc[8:]

    def gram_of(k):
        both = lax.dot_general(left[k], left[k], NT, preferred_element_type=F32)
        both = both[2 * rmax:] + both[rmax:2 * rmax] + both[:rmax]
        return both[:, 2 * rmax:] + both[:, rmax:2 * rmax] + both[:, :rmax]

    def shifted(k, gram):
        rank = ranks_of(k)
        trace = jnp.sum(jnp.where(eye, gram, 0.0), keepdims=True)
        shift = 0.1 * trace / jnp.full((1, 1), rank.astype(F32))
        return gram + jnp.where(
            eye, jnp.where(mat_r < rank, jnp.broadcast_to(shift, (rmax, rmax)), 1.0), 0.0)

    def expand(k, n):
        cols = slice(n * 256, (n + 1) * 256)
        parts = jnp.dot(left[k], low[k, :, cols], preferred_element_type=F32)
        prod[k, :, cols] = parts[:rmax]
        full[k, :, cols] = parts[2 * rmax:] + parts[rmax:2 * rmax] + parts[:rmax]

    def times(a, b):
        a_high, b_high = a.astype(BF16), b.astype(BF16)
        a_low, b_low = (a - a_high.astype(F32)).astype(BF16), (b - b_high.astype(F32)).astype(BF16)
        return jnp.dot(jnp.concatenate([a_high, a_high, a_low], 1), jnp.concatenate([b_high, b_low, b_high], 0),
                       preferred_element_type=F32)

    def solve(jobs, grams):
        mats = [shifted(k, gram) for k, gram in zip(jobs, grams)]
        inverses = invert(mats, [functools.partial(expand, k, n) for k in jobs for n in range(nb // 256)])
        every = []
        for k, inverse in zip(jobs, inverses):
            coeffs = times(inverse, prod[k])
            coef[job_slot[k]] = jnp.where(job_off[k], coeffs, 0.0)
            every.append(coeffs)
            if jobs == (0,):
                sent_c[...] = coeffs.astype(BF16)
        for k, gram, coeffs in zip(jobs, grams, every):
            mixed = coeffs * (times(gram, coeffs) - 2.0 * full[k])
            acc = [jnp.zeros((8, LANES), F32) for _ in range(4)]
            for r in range(0, rmax, 8):
                for cb in range(nb // LANES):
                    acc[cb % 4] = acc[cb % 4] + mixed[r:r + 8, cb * LANES:(cb + 1) * LANES]
            errs[k] = errs[k] + ((acc[0] + acc[1]) + (acc[2] + acc[3]))

    def invert(mats, beside):
        mats = list(mats)
        b = 8
        row8 = lax.broadcasted_iota(jnp.int32, (b, rmax), 0)
        col8 = lax.broadcasted_iota(jnp.int32, (b, rmax), 1)
        for k0 in range(0, rmax, b):
            spread = [[[jnp.broadcast_to(m[i:i + b, k0 + j:k0 + j + 1], (b, rmax)) for j in range(b)]
                       for i in range(0, rmax, b)] for m in mats]
            for todo in beside[k0 // b * len(beside) * b // rmax:(k0 // b + 1) * len(beside) * b // rmax]:
                todo()
            for n in range(len(mats)):
                m = mats[n]
                d = list(spread[n][k0 // b])
                for j in range(b):
                    inverse = 1.0 / d[j][j:j + 1, :]
                    for i in range(b):
                        if i != j:
                            f = d[i][j:j + 1, :] * inverse
                            d[i] = jnp.where(row8 == j, f, d[i] - d[j] * f)
                    d[j] = jnp.where(row8 == j, inverse, -(d[j] * inverse))
                panel = m[k0:k0 + b]
                r = d[0] * panel[0:1]
                for j in range(1, b):
                    r = r + d[j] * panel[j:j + 1]
                for j in range(b):
                    r = jnp.where(col8 == k0 + j, d[j], r)
                inside = (col8 >= k0) & (col8 < k0 + b)
                out = []
                for i in range(0, rmax, b):
                    if i == k0:
                        out.append(r)
                        continue
                    piece = jnp.where(inside, 0.0, m[i:i + b])
                    for j in range(b):
                        piece = piece - spread[n][i // b][j] * r[j:j + 1]
                    out.append(piece)
                mats[n] = jnp.concatenate(out, 0)
        return mats

    def phase_project():
        @pl.when(jnp.logical_not(is_helper))
        def _():
            for k in range(3):
                project(k)

        @pl.when(is_helper)
        def _():
            project(0)
            sent_y[...] = left[0, :rmax]
            gram = gram_of(0)
            back_copies[0]().start()
            solve((0,), [gram])
            back_copies[1]().start()

    def phase_solve():
        @pl.when(jnp.logical_not(is_helper))
        def _():
            jobs = (0, 1, 2)
            grams = [gram_of(k) for k in jobs]
            solve(jobs, grams)

        @pl.when(is_helper)
        def _():
            back_copies[2]().start()
            project(2)
            gram = gram_of(2)
            solve((2,), [gram])

    def wait_z():
        all_of(sums_z.at[0:n_row - 1], sum_recv.at[0])
        plane = sums_z[0]
        for d in range(1, n_row):
            plane = plane + sums_z[d]
        sums_p[q] = plane

    def send_p():
        for d in range(1, n_col):
            p_copy(d).start()

    def phase_far_y():
        @pl.when(is_home)
        def _():
            back_copies[0]().wait_recv()
            wide[3] = far_y[...].astype(F32)
        y_copy.start()

    def phase_far():
        @pl.when(is_home)
        def _():
            for c in back_copies[1:]:
                c().wait_recv()
            coef[3] = far_c[...].astype(F32)
        c_copy.start()

    def total_error():
        all_of(sums_p.at[0:n_col - 1], sum_recv.at[1])
        whole = sums_p[0]
        for d in range(1, n_col):
            whole = whole + sums_p[d]
        total = jnp.sum(whole[0:1, :], keepdims=True)
        rank_out[0] = jnp.sum(whole[1:2, :]).astype(jnp.int32)
        factor = (n_row * slots) / jnp.sqrt(total)
        values = []
        for k in range(3):
            source = jnp.where(job_off[k], errs[k], norms[k])
            value = jnp.sqrt(jnp.maximum(jnp.sum(source, keepdims=True), 0.0)) * factor
            values.append(jnp.where(job_on[k], value, 0.0))
        far = jnp.sqrt(jnp.maximum(jnp.sum(far_err[...], keepdims=True), 0.0)) * factor
        for a in range(slots):
            out = jnp.zeros((1, 1), F32)
            for k in range(3):
                mine = (job_slot[k] == a) & job_on[k]
                if k == 0:
                    mine = mine & jnp.logical_not(is_helper)
                out = jnp.where(mine, values[k], out)
            if a == slots - 1:
                out = jnp.where(is_home, far, out)
            err_out[a] = out[0, 0]

    def wait_sends():
        for g in range(slots - 1):
            @pl.when(sends_group(g))
            def _():
                all_of(row_buf.at[0, 0, 0:LANES], group_send.at[g])
        for d in range(1, 8):
            @pl.when(sends_points(d))
            def _():
                point_copy(d).wait_send()
        all_of(sums_p.at[0:n_col - 1], sum_send.at[1])
        all_of(sums_z.at[0:n_row - 1], sum_send.at[0])
        all_of(bank.at[0:31], bank_send.at[0])

        @pl.when(is_home)
        def _():
            for c in help_copies:
                c().wait_send()

        @pl.when(is_helper)
        def _():
            for c in back_copies:
                c().wait_send()
        y_copy.wait()
        c_copy.wait()

    phase_enter()
    phase_setup()
    order = smooth[0]
    root = jnp.where(order >= 2, math.sqrt(5.0), jnp.where(order >= 1, math.sqrt(3.0), 1.0)).astype(F32)
    scale = (root * LOG2E) / jnp.full((8, LANES), reach[0], F32)
    linear = jnp.where(order >= 1, 1.0 / LOG2E, 0.0).astype(F32)
    square = jnp.where(order >= 2, 1.0 / (3.0 * LOG2E * LOG2E), 0.0).astype(F32)
    phase_barrier()
    phase_points()
    step_own()
    phase_rows(0)
    tile(0, 0, 2)
    step_first(1)
    step_first(3)
    phase_rows(1)
    phase_rows(2)
    tile(0, 2, 4)
    step_first(2)
    tile(0, 4, 8)
    step_second(0)
    tile(1, 0, 4)
    step_second(1)
    tile(1, 4, 8)
    phase_cols()
    step_second(3)
    step_half(0)
    tile(2, 0, 4)
    step_half(1)
    tile(2, 4, 8)
    phase_share()
    step_half(3)
    step_second(2)
    send_z()
    squares(0)
    squares(1)
    squares(2)
    wait_bank()
    phase_project()
    wait_z()
    send_p()
    phase_solve()
    phase_far_y()
    phase_far()
    total_error()
    wait_sends()


def solution(mesh):
    n_row, n_col = mesh.shape["prow"], mesh.shape["pcol"]

    def per_device(points, range_length, smoothness, sketch_bank, sketch_ids, tile_ranks):
        slots = sketch_ids.shape[0]
        nb = points.shape[3]
        rmax = sketch_bank.shape[1]
        dims = (slots, n_row, n_col, nb, rmax)
        anywhere = pl.BlockSpec(memory_space=pl.ANY)
        vmem = pltpu.VMEM
        hbm = pl.BlockSpec(memory_space=pltpu.HBM)
        scalars = pl.BlockSpec(memory_space=pltpu.SMEM)
        smem = pltpu.SMEM
        dma = pltpu.SemaphoreType.DMA
        y_out, c_out, err, rank = pl.pallas_call(
            functools.partial(kernel, dims),
            out_shape=(
                jax.ShapeDtypeStruct((slots, rmax, nb), F32),
                jax.ShapeDtypeStruct((slots, rmax, nb), F32),
                jax.ShapeDtypeStruct((slots,), F32),
                jax.ShapeDtypeStruct((1,), jnp.int32),
            ),
            in_specs=[hbm] * 6,
            out_specs=(anywhere, anywhere, scalars, scalars),
            scratch_shapes=[
                smem((1,), F32), smem((1,), jnp.int32), smem((slots,), jnp.int32), smem((slots,), jnp.int32),
                vmem((2, nb), F32), vmem((slots, 2, nb), F32), vmem((2, nb), F32),
                vmem((n_col, rmax, nb), BF16), vmem((3, nb, nb), BF16),
                vmem((3, 2, nb, LANES), F32), vmem((8, nb), F32), vmem((8, nb), F32),
                vmem((3, 3 * rmax, nb), BF16), vmem((4, rmax, nb), F32), vmem((3, rmax, nb), F32),
                vmem((4, rmax, nb), F32), vmem((3, rmax, nb), F32),
                vmem((3, 8, LANES), F32), vmem((3, 8, LANES), F32),
                vmem((8, LANES), jnp.int32), vmem((8, LANES), jnp.int32),
                vmem((rmax, nb), BF16), vmem((rmax, nb), BF16), vmem((rmax, nb), BF16), vmem((rmax, nb), BF16),
                vmem((8, LANES), F32), vmem((n_row, 8, LANES), F32), vmem((n_col, 8, LANES), F32),
                dma((6,)), dma((3,)), dma((8,)), dma((slots,)), dma((5,)), dma((5,)),
                dma((1,)), dma((4,)), dma((4,)), dma((4,)), dma((1,)), dma((2,)), dma((2,)), dma((2,)),
            ],
            compiler_params=pltpu.CompilerParams(
                collective_id=0, has_side_effects=True, vmem_limit_bytes=VMEM_BYTES),
        )(
            *(pltpu.with_memory_space_constraint(v, pltpu.HBM) for v in (
                points.reshape(2, nb), sketch_bank.reshape(rmax, nb),
                sketch_ids.reshape(slots), tile_ranks.reshape(slots))), range_length, smoothness,
        )
        return (
            y_out.reshape(slots, 1, 1, 1, rmax, nb),
            c_out.reshape(slots, 1, 1, 1, rmax, nb),
            err.reshape(slots, 1, 1, 1),
            rank,
        )

    return jax.shard_map(
        per_device,
        mesh=mesh,
        in_specs=(
            P(None, "pcol", None, None),
            P(),
            P(),
            P("pcol", None, None),
            P(None, "prow", None, "pcol"),
            P(None, "prow", None, "pcol"),
        ),
        out_specs=(
            P(None, "prow", None, "pcol", None, None),
            P(None, "prow", None, "pcol", None, None),
            P(None, "prow", None, "pcol"),
            P(),
        ),
        check_vma=False,
    )
```

```python
import functools
import math

import jax
import jax.numpy as jnp
from jax import lax
from jax.experimental import pallas as pl
from jax.experimental.pallas import tpu as pltpu
from jax.sharding import PartitionSpec as P

MESH = pl.DeviceIdType.MESH
LOG2E = math.log2(math.e)
F32 = jnp.float32
BF16 = jnp.bfloat16
LANES = 128
VMEM_BYTES = 40 * 1024 * 1024
NT = (((1,), (1,)), ((), ()))


def kernel(dims, pts_in, sketch_in, ids_in, ranks_in, reach_in, smooth_in, y_out, c_out, err_out, rank_out,
           reach, smooth, ids, ranks, pts, rows, far_cols, bank, low, row_buf, col_x, col_y, left, wide, prod, coef, full, norms, errs,
           note, far_note, sent_y, sent_c, far_y, far_c, far_err, sums_z, sums_p,
           load_sem, group_send, pts_send, pts_recv, help_send, help_recv, bank_send, bank_recv1, bank_recv2, half_recv, mirror_recv,
           sum_send, sum_recv, out_sem):
    slots, n_row, n_col, nb, rmax = dims
    p = lax.axis_index("prow")
    q = lax.axis_index("pcol")
    y, x, core = q // 8, lax.rem(q // 2, 4), lax.rem(q, 2)
    partner = q + 1 - 2 * core
    turn = lax.rem(q, n_row)
    is_home, is_helper = (y == 0) & (turn <= p), (y == slots - 1) & (turn <= p)
    pair = lax.rem(q + (slots - 1) * n_row, n_col)
    job_slot = (jnp.where(y == 0, 1, slots - 1), jnp.where(y == 2, 1, 2), jnp.where((y == 0) & (turn > p), slots - 1, y))
    job_on = ((y < slots - 1) | is_helper, y <= 1, (y == 0) | (turn <= p))
    job_off = (job_on[0], job_on[1], job_on[2] & (turn != p))

    def remote(src, dst, send, recv, target):
        return pltpu.make_async_remote_copy(src, dst, send, recv, device_id={"pcol": target}, device_id_type=MESH)

    def all_of(ref, sem):
        pltpu.make_async_copy(ref, ref, sem).wait()

    def place(e, f):
        dy = core * e + (1 - core) * f
        dx = (1 - core) * e + core * f
        return lax.rem(y + dy + 8, 4) * 8 + lax.rem(x + dx + 8, 4) * 2 + core

    loads = [pltpu.make_async_copy(src, dst, load_sem.at[i]) for i, (src, dst) in enumerate((
        (ids_in, ids), (ranks_in, ranks), (smooth_in, smooth), (reach_in, reach), (pts_in, pts),
        (sketch_in, bank.at[q])))]
    barrier = pltpu.get_barrier_semaphore()

    def phase_enter():
        for load in loads:
            load.start()
        for d in range(1, n_col):
            pl.semaphore_signal(barrier, inc=1, device_id={"pcol": lax.rem(q + d, n_col)}, device_id_type=MESH)
        for d in range(1, n_row):
            pl.semaphore_signal(barrier, inc=1, device_id={"prow": lax.rem(p + d, n_row)}, device_id_type=MESH)

    lane = lax.broadcasted_iota(jnp.int32, (8, LANES), 1)
    sub = lax.broadcasted_iota(jnp.int32, (8, LANES), 0)

    def phase_setup():
        for load in loads:
            load.wait()
        note[...] = jnp.where(lane == 0, ids[slots - 1], ranks[slots - 1])

    mat_r = lax.broadcasted_iota(jnp.int32, (rmax, rmax), 0)
    mat_c = lax.broadcasted_iota(jnp.int32, (rmax, rmax), 1)
    eye = mat_r == mat_c

    def phase_clear():
        wide[...] = jnp.zeros_like(wide)
        coef[...] = jnp.zeros_like(coef)
        norms[...] = jnp.zeros_like(norms)
        errs[...] = jnp.zeros_like(errs)

    def phase_barrier():
        pl.semaphore_wait(barrier, n_col - 1 + n_row - 1)

    is_source = lax.rem(q, n_row) == p

    def group_copy(g, i):
        return remote(pts, rows.at[y], group_send.at[g], pts_recv.at[y], g * 8 + i)

    def sends_group(g):
        return is_source & (g < y)

    def point_copy(d):
        return remote(pts, rows.at[y], pts_send.at[d], pts_recv.at[y], y * 8 + lax.rem(q + d, 8))

    def sends_points(d):
        return is_source & (turn + d >= 8)

    help_copies = (
        lambda: remote(pts, far_cols, help_send.at[0], help_recv.at[0], pair),
        lambda: remote(note, far_note, help_send.at[1], help_recv.at[1], pair),
    )
    back = lax.rem(q + n_row, n_col)
    back_copies = (
        lambda: remote(sent_y, far_y, help_send.at[2], help_recv.at[2], back),
        lambda: remote(sent_c, far_c, help_send.at[3], help_recv.at[3], back),
        lambda: remote(errs.at[0], far_err, help_send.at[4], help_recv.at[4], back),
    )

    def phase_points():
        for g in range(slots - 1):
            @pl.when(sends_group(g))
            def _():
                for i in range(8):
                    group_copy(g, i).start()
        for d in range(1, 8):
            @pl.when(sends_points(d))
            def _():
                point_copy(d).start()

        @pl.when(is_home)
        def _():
            for c in help_copies:
                c().start()

    def first_copy(d):
        return remote(bank.at[q], bank.at[q], bank_send.at[0], bank_recv1.at[d], place(d, 0))

    def second_copy(e, d):
        block = place(-e, 0)
        return remote(bank.at[block], bank.at[block], bank_send.at[0], bank_recv2.at[e], place(0, d))

    def half_copy(e, d):
        block = place(-e, -d)
        cols = pl.ds(0 if d == 1 else nb // 2, nb // 2)
        return remote(bank.at[block, :, cols], bank.at[block, :, cols], bank_send.at[0], half_recv.at[e], place(0, d))

    def mirror_copy(e, f):
        block = place(-e, -f)
        return remote(bank.at[block], bank.at[block], bank_send.at[0], mirror_recv.at[0], partner)

    def ways(e):
        return (1, 3, 2) if e == 2 else (1, 3)

    def step_near():
        for d in (1, 3):
            first_copy(d).start()

    def step_own():
        first_copy(2).start()
        for d in ways(0):
            second_copy(0, d).start()
        mirror_copy(0, 0).start()

    def step_first(e):
        first_copy(e).wait_recv()
        for d in ways(e):
            second_copy(e, d).start()
        mirror_copy(e, 0).start()

    def step_second(e):
        all_of(bank.at[0:len(ways(e))], bank_recv2.at[e])
        if e != 2:
            for d in (1, 3):
                half_copy(e, d).start()
        for d in ways(e):
            mirror_copy(e, d).start()

    def step_half(e):
        all_of(bank.at[0:1], half_recv.at[e])
        mirror_copy(e, 2).start()

    def prepare_rows(k, source):
        for cb in range(nb // LANES):
            cols = pl.ds(cb * LANES, LANES)
            for c in range(2):
                row_buf[k, c, cols, :] = jnp.broadcast_to(source[c:c + 1, cols] * scale[0:1, :], (LANES, LANES)).T

    def prepare_cols(source):
        for cb in range(nb // LANES):
            cols = pl.ds(cb * LANES, LANES)
            col_x[:, cols] = jnp.broadcast_to(source[0:1, cols], (8, LANES)) * scale
            col_y[:, cols] = jnp.broadcast_to(source[1:2, cols], (8, LANES)) * scale

    def generate(k, buf, g):
        acc = [jnp.zeros((8, LANES), F32) for _ in range(2)]
        for rg in range(LANES // 16):
            r = pl.multiple_of(g * LANES + rg * 16, 16)
            rx = row_buf[buf, 0, pl.ds(r, 16), :]
            ry = row_buf[buf, 1, pl.ds(r, 16), :]
            for cb in range(nb // LANES):
                cols = pl.ds(cb * LANES, LANES)
                cx, cy = col_x[:, cols], col_y[:, cols]
                tiles = []
                for h in range(2):
                    dx = rx[h * 8:h * 8 + 8] - cx
                    dy = ry[h * 8:h * 8 + 8] - cy
                    d2 = jnp.maximum(dx * dx + dy * dy, 1e-30)
                    t = d2 * lax.rsqrt(d2)
                    value = (1.0 + linear * t + square * d2) * jnp.exp2(-t)
                    acc[h] = acc[h] + value * value
                    tiles.append(value)
                low[k, pl.ds(r, 16), cols] = jnp.concatenate(tiles, 0).astype(BF16)
        norms[k] = norms[k] + (acc[0] + acc[1])

    def row_block(k, a):
        @pl.when(q == n_row * a + p)
        def _():
            prepare_rows(k, pts)

        @pl.when(q != n_row * a + p)
        def _():
            remote(pts, rows.at[a], pts_send.at[0], pts_recv.at[a], partner).wait_recv()
            prepare_rows(k, rows.at[a])

    job_rows = (0, 1, jnp.where(is_helper, 0, 2))

    def phase_rows(k):
        if k == 0:
            @pl.when(is_helper)
            def _():
                help_copies[0]().wait_recv()
                help_copies[1]().wait_recv()
                prepare_cols(far_cols)

            @pl.when(jnp.logical_not(is_helper))
            def _():
                prepare_cols(pts)
            for a in (1, slots - 1):
                @pl.when((job_slot[0] == a) & job_on[0])
                def _():
                    row_block(0, a)
        if k == 1:
            @pl.when(job_on[1])
            def _():
                row_block(1, 2)
        if k == 2:
            for a in range(slots):
                @pl.when((job_slot[2] == a) & job_on[2] & jnp.logical_not(is_helper))
                def _():
                    row_block(2, a)

    def phase_cols():
        @pl.when(is_helper)
        def _():
            prepare_cols(pts)

    def tile(k, first, last):
        @pl.when(job_on[k])
        def _():
            def body(g, carry):
                generate(k, job_rows[k], g)
                return carry

            lax.fori_loop(first, last, body, 0)

    def z_copy(d):
        return pltpu.make_async_remote_copy(
            sums_z.at[p, 0:2], sums_z.at[p, 0:2], sum_send.at[0], sum_recv.at[0],
            device_id={"prow": lax.rem(p + d, n_row)}, device_id_type=MESH)

    def p_copy(d):
        return remote(sums_p.at[q, 0:2], sums_p.at[q, 0:2], sum_send.at[1], sum_recv.at[1], lax.rem(q + d, n_col))

    def phase_share():
        share = jnp.zeros((8, LANES), F32)
        for k in range(3):
            weight = jnp.where(job_off[k], 2.0, jnp.where(job_on[k], 1.0, 0.0)).astype(F32)
            share = share + weight * norms[k]
        rank_share = jnp.int32(0)
        for a in range(slots):
            rank_share = rank_share + jnp.where(q < n_row * a + p, ranks[a], 0)
        folded = jnp.sum(share, axis=0, keepdims=True)
        sums_z[p] = jnp.where(sub == 0, jnp.broadcast_to(folded, (8, LANES)),
                              jnp.where((sub == 1) & (lane == 0), rank_share.astype(F32), 0.0))

    def wait_bank():
        all_of(bank.at[0:16], mirror_recv.at[0])

    def send_z():
        for d in range(1, n_row):
            z_copy(d).start()

    y_copy = pltpu.make_async_copy(wide, y_out, out_sem.at[0])
    c_copy = pltpu.make_async_copy(coef, c_out, out_sem.at[1])

    def ranks_of(k):
        own = ranks[job_slot[k]]
        return jnp.where(is_helper, far_note[0:1, 1:2][0, 0], own) if k == 0 else own

    def id_of(k):
        own = ids[job_slot[k]]
        return jnp.where(is_helper, far_note[0:1, 0:1][0, 0], own) if k == 0 else own

    def project(k):
        rank = ranks_of(k)
        keep = lax.broadcasted_iota(jnp.int32, (rmax, nb), 0) < rank
        chosen = jnp.where(keep, bank[id_of(k)].astype(F32), 0.0).astype(BF16)
        acc = [jnp.zeros((16, LANES), F32) for _ in range(4)]
        width = 256
        for n in range(nb // width):
            cols = slice(n * width, (n + 1) * width)
            sketched = lax.dot_general(chosen, low[k, cols, :], NT, preferred_element_type=F32)
            high = sketched.astype(BF16)
            rest = sketched - high.astype(F32)
            middle = rest.astype(BF16)
            left[k, :, cols] = jnp.concatenate([high, middle, (rest - middle.astype(F32)).astype(BF16)], 0)
            wide[job_slot[k], :, cols] = jnp.where(job_off[k], sketched, 0.0)
            for r in range(n * width, (n + 1) * width, 16):
                for cb in range(nb // LANES):
                    value = low[k, r:r + 16, cb * LANES:(cb + 1) * LANES].astype(F32)
                    acc[cb % 4] = acc[cb % 4] + value * value
        acc = (acc[0] + acc[1]) + (acc[2] + acc[3])
        errs[k] = acc[:8] + acc[8:]

    def gram_of(k):
        both = lax.dot_general(left[k], left[k], NT, preferred_element_type=F32)
        both = both[2 * rmax:] + both[rmax:2 * rmax] + both[:rmax]
        return both[:, 2 * rmax:] + both[:, rmax:2 * rmax] + both[:, :rmax]

    def shifted(k, gram):
        rank = ranks_of(k)
        trace = jnp.sum(jnp.where(eye, gram, 0.0), keepdims=True)
        shift = 0.1 * trace / jnp.full((1, 1), rank.astype(F32))
        return gram + jnp.where(
            eye, jnp.where(mat_r < rank, jnp.broadcast_to(shift, (rmax, rmax)), 1.0), 0.0)

    def expand(k, n):
        cols = slice(n * 256, (n + 1) * 256)
        parts = jnp.dot(left[k], low[k, :, cols], preferred_element_type=F32)
        prod[k, :, cols] = parts[:rmax]
        full[k, :, cols] = parts[2 * rmax:] + parts[rmax:2 * rmax] + parts[:rmax]

    def times(a, b):
        a_high, b_high = a.astype(BF16), b.astype(BF16)
        a_low, b_low = (a - a_high.astype(F32)).astype(BF16), (b - b_high.astype(F32)).astype(BF16)
        return jnp.dot(jnp.concatenate([a_high, a_high, a_low], 1), jnp.concatenate([b_high, b_low, b_high], 0),
                       preferred_element_type=F32)

    def solve(jobs, grams, ready=None):
        mats = [shifted(k, gram) for k, gram in zip(jobs, grams)]
        inverses = invert(mats, [functools.partial(expand, k, n) for k in jobs for n in range(nb // 256)])
        every = []
        for k, inverse in zip(jobs, inverses):
            coeffs = times(inverse, prod[k])
            coef[job_slot[k]] = jnp.where(job_off[k], coeffs, 0.0)
            every.append(coeffs)
            if jobs == (0,):
                sent_c[...] = coeffs.astype(BF16)
        for k, gram, coeffs in zip(jobs, grams, every):
            mixed = coeffs * (times(gram, coeffs) - 2.0 * full[k])
            if ready is not None:
                ready()
            acc = [jnp.zeros((8, LANES), F32) for _ in range(4)]
            for r in range(0, rmax, 8):
                for cb in range(nb // LANES):
                    acc[cb % 4] = acc[cb % 4] + mixed[r:r + 8, cb * LANES:(cb + 1) * LANES]
            errs[k] = errs[k] + ((acc[0] + acc[1]) + (acc[2] + acc[3]))

    def invert(mats, beside):
        mats = list(mats)
        b = 8
        row8 = lax.broadcasted_iota(jnp.int32, (b, rmax), 0)
        col8 = lax.broadcasted_iota(jnp.int32, (b, rmax), 1)
        for k0 in range(0, rmax, b):
            spread = [[[jnp.broadcast_to(m[i:i + b, k0 + j:k0 + j + 1], (b, rmax)) for j in range(b)]
                       for i in range(0, rmax, b)] for m in mats]
            for todo in beside[k0 // b * len(beside) * b // rmax:(k0 // b + 1) * len(beside) * b // rmax]:
                todo()
            for n in range(len(mats)):
                m = mats[n]
                d = list(spread[n][k0 // b])
                for j in range(b):
                    inverse = 1.0 / d[j][j:j + 1, :]
                    for i in range(b):
                        if i != j:
                            f = d[i][j:j + 1, :] * inverse
                            d[i] = jnp.where(row8 == j, f, d[i] - d[j] * f)
                    d[j] = jnp.where(row8 == j, inverse, -(d[j] * inverse))
                panel = m[k0:k0 + b]
                r = d[0] * panel[0:1]
                for j in range(1, b):
                    r = r + d[j] * panel[j:j + 1]
                for j in range(b):
                    r = jnp.where(col8 == k0 + j, d[j], r)
                inside = (col8 >= k0) & (col8 < k0 + b)
                out = []
                for i in range(0, rmax, b):
                    if i == k0:
                        out.append(r)
                        continue
                    piece = jnp.where(inside, 0.0, m[i:i + b])
                    for j in range(b):
                        piece = piece - spread[n][i // b][j] * r[j:j + 1]
                    out.append(piece)
                mats[n] = jnp.concatenate(out, 0)
        return mats

    def phase_project():
        @pl.when(jnp.logical_not(is_helper))
        def _():
            for k in range(3):
                project(k)

        @pl.when(is_helper)
        def _():
            project(0)
            sent_y[...] = left[0, :rmax]
            gram = gram_of(0)
            back_copies[0]().start()
            solve((0,), [gram], lambda: back_copies[1]().start())

    def phase_solve():
        @pl.when(jnp.logical_not(is_helper))
        def _():
            jobs = (0, 1, 2)
            grams = [gram_of(k) for k in jobs]
            solve(jobs, grams)

        @pl.when(is_helper)
        def _():
            back_copies[2]().start()
            project(2)
            gram = gram_of(2)
            solve((2,), [gram])

    def wait_z():
        all_of(sums_z.at[0:n_row - 1, 0:2], sum_recv.at[0])
        plane = sums_z[0, 0:2]
        for d in range(1, n_row):
            plane = plane + sums_z[d, 0:2]
        sums_p[q, 0:2] = plane

    def send_p():
        for d in range(1, n_col):
            p_copy(d).start()

    def phase_far_y():
        @pl.when(is_home)
        def _():
            back_copies[0]().wait_recv()
            wide[3] = far_y[...].astype(F32)
        y_copy.start()

    def phase_far():
        @pl.when(is_home)
        def _():
            for c in back_copies[1:]:
                c().wait_recv()
            coef[3] = far_c[...].astype(F32)
        c_copy.start()

    def total_error():
        all_of(sums_p.at[0:n_col - 1, 0:2], sum_recv.at[1])
        whole = sums_p[0, 0:2]
        for d in range(1, n_col):
            whole = whole + sums_p[d, 0:2]
        total = jnp.sum(whole[0:1, :], keepdims=True)
        rank_out[0] = jnp.sum(whole[1:2, :]).astype(jnp.int32)
        factor = (n_row * slots) / jnp.sqrt(total)
        values = []
        for k in range(3):
            source = jnp.where(job_off[k], errs[k], norms[k])
            value = jnp.sqrt(jnp.maximum(jnp.sum(source, keepdims=True), 0.0)) * factor
            values.append(jnp.where(job_on[k], value, 0.0))
        far = jnp.sqrt(jnp.maximum(jnp.sum(far_err[...], keepdims=True), 0.0)) * factor
        for a in range(slots):
            out = jnp.zeros((1, 1), F32)
            for k in range(3):
                mine = (job_slot[k] == a) & job_on[k]
                if k == 0:
                    mine = mine & jnp.logical_not(is_helper)
                out = jnp.where(mine, values[k], out)
            if a == slots - 1:
                out = jnp.where(is_home, far, out)
            err_out[a] = out[0, 0]

    def wait_sends():
        for g in range(slots - 1):
            @pl.when(sends_group(g))
            def _():
                all_of(row_buf.at[0, 0, 0:LANES], group_send.at[g])
        for d in range(1, 8):
            @pl.when(sends_points(d))
            def _():
                point_copy(d).wait_send()
        all_of(sums_p.at[0:n_col - 1, 0:2], sum_send.at[1])
        all_of(sums_z.at[0:n_row - 1, 0:2], sum_send.at[0])
        all_of(bank.at[0:31], bank_send.at[0])

        @pl.when(is_home)
        def _():
            for c in help_copies:
                c().wait_send()
            remote(pts, rows.at[slots - 1], pts_send.at[0], pts_recv.at[slots - 1], partner).wait_recv()

        @pl.when(is_helper)
        def _():
            for c in back_copies:
                c().wait_send()
        y_copy.wait()
        c_copy.wait()

    phase_enter()
    phase_setup()
    order = smooth[0]
    root = jnp.where(order >= 2, math.sqrt(5.0), jnp.where(order >= 1, math.sqrt(3.0), 1.0)).astype(F32)
    scale = (root * LOG2E) / jnp.full((8, LANES), reach[0], F32)
    linear = jnp.where(order >= 1, 1.0 / LOG2E, 0.0).astype(F32)
    square = jnp.where(order >= 2, 1.0 / (3.0 * LOG2E * LOG2E), 0.0).astype(F32)
    phase_barrier()
    step_near()
    phase_points()
    phase_clear()
    step_own()
    step_first(1)
    step_first(3)
    phase_rows(0)
    tile(0, 0, 2)
    phase_rows(1)
    phase_rows(2)
    step_first(2)
    tile(0, 2, 4)
    step_second(0)
    tile(0, 4, 8)
    tile(1, 0, 2)
    step_second(1)
    tile(1, 2, 4)
    step_second(3)
    tile(1, 4, 8)
    phase_cols()
    tile(2, 0, 2)
    step_half(0)
    step_second(2)
    tile(2, 2, 4)
    step_half(1)
    tile(2, 4, 6)
    step_half(3)
    tile(2, 6, 8)
    phase_share()
    send_z()
    wait_bank()
    phase_project()
    wait_z()
    send_p()
    phase_solve()
    phase_far_y()
    phase_far()
    total_error()
    wait_sends()


def solution(mesh):
    n_row, n_col = mesh.shape["prow"], mesh.shape["pcol"]

    def per_device(points, range_length, smoothness, sketch_bank, sketch_ids, tile_ranks):
        slots = sketch_ids.shape[0]
        nb = points.shape[3]
        rmax = sketch_bank.shape[1]
        dims = (slots, n_row, n_col, nb, rmax)
        anywhere = pl.BlockSpec(memory_space=pl.ANY)
        vmem = pltpu.VMEM
        hbm = pl.BlockSpec(memory_space=pltpu.HBM)
        scalars = pl.BlockSpec(memory_space=pltpu.SMEM)
        smem = pltpu.SMEM
        dma = pltpu.SemaphoreType.DMA
        y_out, c_out, err, rank = pl.pallas_call(
            functools.partial(kernel, dims),
            out_shape=(
                jax.ShapeDtypeStruct((slots, rmax, nb), F32),
                jax.ShapeDtypeStruct((slots, rmax, nb), F32),
                jax.ShapeDtypeStruct((slots,), F32),
                jax.ShapeDtypeStruct((1,), jnp.int32),
            ),
            in_specs=[hbm] * 6,
            out_specs=(anywhere, anywhere, scalars, scalars),
            scratch_shapes=[
                smem((1,), F32), smem((1,), jnp.int32), smem((slots,), jnp.int32), smem((slots,), jnp.int32),
                vmem((2, nb), F32), vmem((slots, 2, nb), F32), vmem((2, nb), F32),
                vmem((n_col, rmax, nb), BF16), vmem((3, nb, nb), BF16),
                vmem((3, 2, nb, LANES), F32), vmem((8, nb), F32), vmem((8, nb), F32),
                vmem((3, 3 * rmax, nb), BF16), vmem((4, rmax, nb), F32), vmem((3, rmax, nb), F32),
                vmem((4, rmax, nb), F32), vmem((3, rmax, nb), F32),
                vmem((3, 8, LANES), F32), vmem((3, 8, LANES), F32),
                vmem((8, LANES), jnp.int32), vmem((8, LANES), jnp.int32),
                vmem((rmax, nb), BF16), vmem((rmax, nb), BF16), vmem((rmax, nb), BF16), vmem((rmax, nb), BF16),
                vmem((8, LANES), F32), vmem((n_row, 8, LANES), F32), vmem((n_col, 8, LANES), F32),
                dma((6,)), dma((3,)), dma((8,)), dma((slots,)), dma((5,)), dma((5,)),
                dma((1,)), dma((4,)), dma((4,)), dma((4,)), dma((1,)), dma((2,)), dma((2,)), dma((2,)),
            ],
            compiler_params=pltpu.CompilerParams(
                collective_id=0, has_side_effects=True, vmem_limit_bytes=VMEM_BYTES),
        )(
            *(pltpu.with_memory_space_constraint(v, pltpu.HBM) for v in (
                points.reshape(2, nb), sketch_bank.reshape(rmax, nb),
                sketch_ids.reshape(slots), tile_ranks.reshape(slots))), range_length, smoothness,
        )
        return (
            y_out.reshape(slots, 1, 1, 1, rmax, nb),
            c_out.reshape(slots, 1, 1, 1, rmax, nb),
            err.reshape(slots, 1, 1, 1),
            rank,
        )

    return jax.shard_map(
        per_device,
        mesh=mesh,
        in_specs=(
            P(None, "pcol", None, None),
            P(),
            P(),
            P("pcol", None, None),
            P(None, "prow", None, "pcol"),
            P(None, "prow", None, "pcol"),
        ),
        out_specs=(
            P(None, "prow", None, "pcol", None, None),
            P(None, "prow", None, "pcol", None, None),
            P(None, "prow", None, "pcol"),
            P(),
        ),
        check_vma=False,
    )
```

```python
import functools
import math

import jax
import jax.numpy as jnp
from jax import lax
from jax.experimental import pallas as pl
from jax.experimental.pallas import tpu as pltpu
from jax.sharding import PartitionSpec as P

MESH = pl.DeviceIdType.MESH
LOG2E = math.log2(math.e)
F32 = jnp.float32
BF16 = jnp.bfloat16
LANES = 128
VMEM_BYTES = 40 * 1024 * 1024
NT = (((1,), (1,)), ((), ()))


def kernel(dims, pts_in, sketch_in, ids_in, ranks_in, reach_in, smooth_in, y_out, c_out, err_out, rank_out,
           reach, smooth, ids, ranks, pts, rows, far_cols, bank, low, row_buf, col_x, col_y, left, wide, prod, coef, full, grams, norms, errs,
           note, far_note, sent_y, sent_c, far_y, far_c, far_err, sums_z, sums_p,
           load_sem, group_send, pts_send, pts_recv, help_send, help_recv, bank_send, bank_recv1, bank_recv2, half_recv, mirror_recv,
           sum_send, sum_recv, out_sem):
    slots, n_row, n_col, nb, rmax = dims
    p = lax.axis_index("prow")
    q = lax.axis_index("pcol")
    y, x, core = q // 8, lax.rem(q // 2, 4), lax.rem(q, 2)
    partner = q + 1 - 2 * core
    turn = lax.rem(q, n_row)
    is_home, is_helper = (y == 0) & (turn <= p), (y == slots - 1) & (turn <= p)
    pair = lax.rem(q + (slots - 1) * n_row, n_col)
    job_slot = (jnp.where(y == 0, 1, slots - 1), jnp.where(y == 2, 1, 2), jnp.where((y == 0) & (turn > p), slots - 1, y))
    job_on = ((y < slots - 1) | is_helper, y <= 1, (y == 0) | (turn <= p))
    job_off = (job_on[0], job_on[1], job_on[2] & (turn != p))

    def remote(src, dst, send, recv, target):
        return pltpu.make_async_remote_copy(src, dst, send, recv, device_id={"pcol": target}, device_id_type=MESH)

    def all_of(ref, sem):
        pltpu.make_async_copy(ref, ref, sem).wait()

    def place(e, f):
        dy = core * e + (1 - core) * f
        dx = (1 - core) * e + core * f
        return lax.rem(y + dy + 8, 4) * 8 + lax.rem(x + dx + 8, 4) * 2 + core

    loads = [pltpu.make_async_copy(src, dst, load_sem.at[i]) for i, (src, dst) in enumerate((
        (ids_in, ids), (ranks_in, ranks), (smooth_in, smooth), (reach_in, reach), (pts_in, pts),
        (sketch_in, bank.at[q])))]
    barrier = pltpu.get_barrier_semaphore()

    def phase_enter():
        for load in loads:
            load.start()
        for d in range(1, n_col):
            pl.semaphore_signal(barrier, inc=1, device_id={"pcol": lax.rem(q + d, n_col)}, device_id_type=MESH)
        for d in range(1, n_row):
            pl.semaphore_signal(barrier, inc=1, device_id={"prow": lax.rem(p + d, n_row)}, device_id_type=MESH)

    lane = lax.broadcasted_iota(jnp.int32, (8, LANES), 1)
    sub = lax.broadcasted_iota(jnp.int32, (8, LANES), 0)

    def phase_setup():
        for load in loads:
            load.wait()
        note[...] = jnp.where(lane == 0, ids[slots - 1], ranks[slots - 1])

    mat_r = lax.broadcasted_iota(jnp.int32, (rmax, rmax), 0)
    mat_c = lax.broadcasted_iota(jnp.int32, (rmax, rmax), 1)
    eye = mat_r == mat_c

    def phase_clear():
        wide[...] = jnp.zeros_like(wide)
        coef[...] = jnp.zeros_like(coef)
        norms[...] = jnp.zeros_like(norms)
        errs[...] = jnp.zeros_like(errs)

    def phase_barrier():
        pl.semaphore_wait(barrier, n_col - 1 + n_row - 1)

    is_source = lax.rem(q, n_row) == p

    def group_copy(g, i):
        return remote(pts, rows.at[y], group_send.at[g], pts_recv.at[y], g * 8 + i)

    def sends_group(g):
        return is_source & (g < y)

    def point_copy(d):
        return remote(pts, rows.at[y], pts_send.at[d], pts_recv.at[y], y * 8 + lax.rem(q + d, 8))

    def sends_points(d):
        return is_source & (turn + d >= 8)

    help_copies = (
        lambda: remote(pts, far_cols, help_send.at[0], help_recv.at[0], pair),
        lambda: remote(note, far_note, help_send.at[1], help_recv.at[1], pair),
    )
    back = lax.rem(q + n_row, n_col)
    back_copies = (
        lambda: remote(sent_y, far_y, help_send.at[2], help_recv.at[2], back),
        lambda: remote(sent_c, far_c, help_send.at[3], help_recv.at[3], back),
        lambda: remote(errs.at[0], far_err, help_send.at[4], help_recv.at[4], back),
    )

    def phase_points():
        for g in range(slots - 1):
            @pl.when(sends_group(g))
            def _():
                for i in range(8):
                    group_copy(g, i).start()
        for d in range(1, 8):
            @pl.when(sends_points(d))
            def _():
                point_copy(d).start()

        @pl.when(is_home)
        def _():
            for c in help_copies:
                c().start()

    def first_copy(d):
        return remote(bank.at[q], bank.at[q], bank_send.at[0], bank_recv1.at[d], place(d, 0))

    def second_copy(e, d):
        block = place(-e, 0)
        return remote(bank.at[block], bank.at[block], bank_send.at[0], bank_recv2.at[e], place(0, d))

    def half_copy(e, d):
        block = place(-e, -d)
        cols = pl.ds(0 if d == 1 else nb // 2, nb // 2)
        return remote(bank.at[block, :, cols], bank.at[block, :, cols], bank_send.at[0], half_recv.at[e], place(0, d))

    def mirror_copy(e, f):
        block = place(-e, -f)
        return remote(bank.at[block], bank.at[block], bank_send.at[0], mirror_recv.at[0], partner)

    def ways(e):
        return (1, 3, 2) if e == 2 else (1, 3)

    def step_near():
        for d in (1, 3):
            first_copy(d).start()

    def step_own():
        first_copy(2).start()
        for d in ways(0):
            second_copy(0, d).start()
        mirror_copy(0, 0).start()

    def step_first(e):
        first_copy(e).wait_recv()
        for d in ways(e):
            second_copy(e, d).start()
        mirror_copy(e, 0).start()

    def step_second(e):
        all_of(bank.at[0:len(ways(e))], bank_recv2.at[e])
        if e != 2:
            for d in (1, 3):
                half_copy(e, d).start()
        for d in ways(e):
            mirror_copy(e, d).start()

    def step_half(e):
        all_of(bank.at[0:1], half_recv.at[e])
        mirror_copy(e, 2).start()

    def prepare_rows(k, source):
        for cb in range(nb // LANES):
            cols = pl.ds(cb * LANES, LANES)
            for c in range(2):
                row_buf[k, c, cols, :] = jnp.broadcast_to(source[c:c + 1, cols] * scale[0:1, :], (LANES, LANES)).T

    def prepare_cols(source):
        for cb in range(nb // LANES):
            cols = pl.ds(cb * LANES, LANES)
            col_x[:, cols] = jnp.broadcast_to(source[0:1, cols], (8, LANES)) * scale
            col_y[:, cols] = jnp.broadcast_to(source[1:2, cols], (8, LANES)) * scale

    def generate(k, buf, g):
        acc = [jnp.zeros((8, LANES), F32) for _ in range(2)]
        for rg in range(LANES // 16):
            r = pl.multiple_of(g * LANES + rg * 16, 16)
            rx = row_buf[buf, 0, pl.ds(r, 16), :]
            ry = row_buf[buf, 1, pl.ds(r, 16), :]
            for cb in range(nb // LANES):
                cols = pl.ds(cb * LANES, LANES)
                cx, cy = col_x[:, cols], col_y[:, cols]
                tiles = []
                for h in range(2):
                    dx = rx[h * 8:h * 8 + 8] - cx
                    dy = ry[h * 8:h * 8 + 8] - cy
                    d2 = jnp.maximum(dx * dx + dy * dy, 1e-30)
                    t = d2 * lax.rsqrt(d2)
                    value = (1.0 + linear * t + square * d2) * jnp.exp2(-t)
                    acc[h] = acc[h] + value * value
                    tiles.append(value)
                low[k, pl.ds(r, 16), cols] = jnp.concatenate(tiles, 0).astype(BF16)
        norms[k] = norms[k] + (acc[0] + acc[1])

    def row_block(k, a):
        @pl.when(q == n_row * a + p)
        def _():
            prepare_rows(k, pts)

        @pl.when(q != n_row * a + p)
        def _():
            remote(pts, rows.at[a], pts_send.at[0], pts_recv.at[a], partner).wait_recv()
            prepare_rows(k, rows.at[a])

    job_rows = (0, 1, jnp.where(is_helper, 0, 2))

    def phase_rows(k):
        if k == 0:
            @pl.when(is_helper)
            def _():
                help_copies[0]().wait_recv()
                help_copies[1]().wait_recv()
                prepare_cols(far_cols)

            @pl.when(jnp.logical_not(is_helper))
            def _():
                prepare_cols(pts)
            for a in (1, slots - 1):
                @pl.when((job_slot[0] == a) & job_on[0])
                def _():
                    row_block(0, a)
        if k == 1:
            @pl.when(job_on[1])
            def _():
                row_block(1, 2)
        if k == 2:
            for a in range(slots):
                @pl.when((job_slot[2] == a) & job_on[2] & jnp.logical_not(is_helper))
                def _():
                    row_block(2, a)

    def phase_cols():
        @pl.when(is_helper)
        def _():
            prepare_cols(pts)

    def tile(k, first, last):
        @pl.when(job_on[k])
        def _():
            def body(g, carry):
                generate(k, job_rows[k], g)
                return carry

            lax.fori_loop(first, last, body, 0)

    def z_copy(d):
        return pltpu.make_async_remote_copy(
            sums_z.at[p, 0:2], sums_z.at[p, 0:2], sum_send.at[0], sum_recv.at[0],
            device_id={"prow": lax.rem(p + d, n_row)}, device_id_type=MESH)

    def p_copy(d):
        return remote(sums_p.at[q, 0:2], sums_p.at[q, 0:2], sum_send.at[1], sum_recv.at[1], lax.rem(q + d, n_col))

    def phase_share():
        share = jnp.zeros((8, LANES), F32)
        for k in range(3):
            weight = jnp.where(job_off[k], 2.0, jnp.where(job_on[k], 1.0, 0.0)).astype(F32)
            share = share + weight * norms[k]
        rank_share = jnp.int32(0)
        for a in range(slots):
            rank_share = rank_share + jnp.where(q < n_row * a + p, ranks[a], 0)
        folded = jnp.sum(share, axis=0, keepdims=True)
        sums_z[p] = jnp.where(sub == 0, jnp.broadcast_to(folded, (8, LANES)),
                              jnp.where((sub == 1) & (lane == 0), rank_share.astype(F32), 0.0))

    def wait_bank():
        all_of(bank.at[0:16], mirror_recv.at[0])

    def send_z():
        for d in range(1, n_row):
            z_copy(d).start()

    y_copy = pltpu.make_async_copy(wide, y_out, out_sem.at[0])
    c_copy = pltpu.make_async_copy(coef, c_out, out_sem.at[1])

    def ranks_of(k):
        own = ranks[job_slot[k]]
        return jnp.where(is_helper, far_note[0:1, 1:2][0, 0], own) if k == 0 else own

    def id_of(k):
        own = ids[job_slot[k]]
        return jnp.where(is_helper, far_note[0:1, 0:1][0, 0], own) if k == 0 else own

    def project(k):
        rank = ranks_of(k)
        keep = lax.broadcasted_iota(jnp.int32, (rmax, nb), 0) < rank
        chosen = jnp.where(keep, bank[id_of(k)].astype(F32), 0.0).astype(BF16)
        acc = [jnp.zeros((16, LANES), F32) for _ in range(4)]
        width = 256
        for n in range(nb // width):
            cols = slice(n * width, (n + 1) * width)
            sketched = lax.dot_general(chosen, low[k, cols, :], NT, preferred_element_type=F32)
            high = sketched.astype(BF16)
            rest = sketched - high.astype(F32)
            middle = rest.astype(BF16)
            left[k, :, cols] = jnp.concatenate([high, middle, (rest - middle.astype(F32)).astype(BF16)], 0)
            wide[job_slot[k], :, cols] = jnp.where(job_off[k], sketched, 0.0)
            for r in range(n * width, (n + 1) * width, 16):
                for cb in range(nb // LANES):
                    value = low[k, r:r + 16, cb * LANES:(cb + 1) * LANES].astype(F32)
                    acc[cb % 4] = acc[cb % 4] + value * value
        acc = (acc[0] + acc[1]) + (acc[2] + acc[3])
        errs[k] = acc[:8] + acc[8:]

    def gram_of(k):
        both = lax.dot_general(left[k], left[k], NT, preferred_element_type=F32)
        both = both[2 * rmax:] + both[rmax:2 * rmax] + both[:rmax]
        return both[:, 2 * rmax:] + both[:, rmax:2 * rmax] + both[:, :rmax]

    def shifted(k, gram):
        rank = ranks_of(k)
        trace = jnp.sum(jnp.where(eye, gram, 0.0), keepdims=True)
        shift = 0.1 * trace / jnp.full((1, 1), rank.astype(F32))
        return gram + jnp.where(
            eye, jnp.where(mat_r < rank, jnp.broadcast_to(shift, (rmax, rmax)), 1.0), 0.0)

    def expand(k, n):
        cols = slice(n * 256, (n + 1) * 256)
        parts = jnp.dot(left[k], low[k, :, cols], preferred_element_type=F32)
        prod[k, :, cols] = parts[:rmax]
        full[k, :, cols] = parts[2 * rmax:] + parts[rmax:2 * rmax] + parts[:rmax]

    def times(a, b):
        a_high, b_high = a.astype(BF16), b.astype(BF16)
        a_low, b_low = (a - a_high.astype(F32)).astype(BF16), (b - b_high.astype(F32)).astype(BF16)
        return jnp.dot(jnp.concatenate([a_high, a_high, a_low], 1), jnp.concatenate([b_high, b_low, b_high], 0),
                       preferred_element_type=F32)

    def keep_gram(k):
        gram = gram_of(k)
        grams[0, k] = gram
        grams[1, k] = shifted(k, gram)

    def solve(jobs, plain, mats, ready=None):
        inverses = invert(mats, [functools.partial(expand, k, n) for k in jobs for n in range(nb // 256)])
        every = []
        for k, inverse in zip(jobs, inverses):
            coeffs = times(inverse, prod[k])
            coef[job_slot[k]] = jnp.where(job_off[k], coeffs, 0.0)
            every.append(coeffs)
            if jobs == (0,):
                sent_c[...] = coeffs.astype(BF16)
        for k, gram, coeffs in zip(jobs, plain, every):
            mixed = coeffs * (times(gram, coeffs) - 2.0 * full[k])
            if ready is not None:
                ready()
            acc = [jnp.zeros((8, LANES), F32) for _ in range(4)]
            for r in range(0, rmax, 8):
                for cb in range(nb // LANES):
                    acc[cb % 4] = acc[cb % 4] + mixed[r:r + 8, cb * LANES:(cb + 1) * LANES]
            errs[k] = errs[k] + ((acc[0] + acc[1]) + (acc[2] + acc[3]))

    def invert(mats, beside):
        mats = list(mats)
        b = 8
        row8 = lax.broadcasted_iota(jnp.int32, (b, rmax), 0)
        col8 = lax.broadcasted_iota(jnp.int32, (b, rmax), 1)
        for k0 in range(0, rmax, b):
            spread = [[[jnp.broadcast_to(m[i:i + b, k0 + j:k0 + j + 1], (b, rmax)) for j in range(b)]
                       for i in range(0, rmax, b)] for m in mats]
            for todo in beside[k0 // b * len(beside) * b // rmax:(k0 // b + 1) * len(beside) * b // rmax]:
                todo()
            for n in range(len(mats)):
                m = mats[n]
                d = list(spread[n][k0 // b])
                for j in range(b):
                    inverse = 1.0 / d[j][j:j + 1, :]
                    for i in range(b):
                        if i != j:
                            f = d[i][j:j + 1, :] * inverse
                            d[i] = jnp.where(row8 == j, f, d[i] - d[j] * f)
                    d[j] = jnp.where(row8 == j, inverse, -(d[j] * inverse))
                panel = m[k0:k0 + b]
                r = d[0] * panel[0:1]
                for j in range(1, b):
                    r = r + d[j] * panel[j:j + 1]
                for j in range(b):
                    r = jnp.where(col8 == k0 + j, d[j], r)
                inside = (col8 >= k0) & (col8 < k0 + b)
                out = []
                for i in range(0, rmax, b):
                    if i == k0:
                        out.append(r)
                        continue
                    piece = jnp.where(inside, 0.0, m[i:i + b])
                    for j in range(b):
                        piece = piece - spread[n][i // b][j] * r[j:j + 1]
                    out.append(piece)
                mats[n] = jnp.concatenate(out, 0)
        return mats

    def phase_project():
        @pl.when(jnp.logical_not(is_helper))
        def _():
            project(0)
            project(1)
            keep_gram(0)
            project(2)
            keep_gram(1)
            keep_gram(2)

        @pl.when(is_helper)
        def _():
            project(0)
            sent_y[...] = left[0, :rmax]
            gram = gram_of(0)
            back_copies[0]().start()
            solve((0,), [gram], [shifted(0, gram)], lambda: back_copies[1]().start())

    def phase_solve():
        @pl.when(jnp.logical_not(is_helper))
        def _():
            jobs = (0, 1, 2)
            solve(jobs, [grams[0, k] for k in jobs], [grams[1, k] for k in jobs])

        @pl.when(is_helper)
        def _():
            back_copies[2]().start()
            project(2)
            gram = gram_of(2)
            solve((2,), [gram], [shifted(2, gram)])

    def wait_z():
        all_of(sums_z.at[0:n_row - 1, 0:2], sum_recv.at[0])
        plane = sums_z[0, 0:2]
        for d in range(1, n_row):
            plane = plane + sums_z[d, 0:2]
        sums_p[q, 0:2] = plane

    def send_p():
        for d in range(1, n_col):
            p_copy(d).start()

    def phase_far_y():
        @pl.when(is_home)
        def _():
            back_copies[0]().wait_recv()
            wide[3] = far_y[...].astype(F32)
        y_copy.start()

    def phase_far():
        @pl.when(is_home)
        def _():
            for c in back_copies[1:]:
                c().wait_recv()
            coef[3] = far_c[...].astype(F32)
        c_copy.start()

    def total_error():
        all_of(sums_p.at[0:n_col - 1, 0:2], sum_recv.at[1])
        whole = sums_p[0, 0:2]
        for d in range(1, n_col):
            whole = whole + sums_p[d, 0:2]
        total = jnp.sum(whole[0:1, :], keepdims=True)
        rank_out[0] = jnp.sum(whole[1:2, :]).astype(jnp.int32)
        factor = (n_row * slots) / jnp.sqrt(total)
        values = []
        for k in range(3):
            source = jnp.where(job_off[k], errs[k], norms[k])
            value = jnp.sqrt(jnp.maximum(jnp.sum(source, keepdims=True), 0.0)) * factor
            values.append(jnp.where(job_on[k], value, 0.0))
        far = jnp.sqrt(jnp.maximum(jnp.sum(far_err[...], keepdims=True), 0.0)) * factor
        for a in range(slots):
            out = jnp.zeros((1, 1), F32)
            for k in range(3):
                mine = (job_slot[k] == a) & job_on[k]
                if k == 0:
                    mine = mine & jnp.logical_not(is_helper)
                out = jnp.where(mine, values[k], out)
            if a == slots - 1:
                out = jnp.where(is_home, far, out)
            err_out[a] = out[0, 0]

    def wait_sends():
        for g in range(slots - 1):
            @pl.when(sends_group(g))
            def _():
                all_of(row_buf.at[0, 0, 0:LANES], group_send.at[g])
        for d in range(1, 8):
            @pl.when(sends_points(d))
            def _():
                point_copy(d).wait_send()
        all_of(sums_p.at[0:n_col - 1, 0:2], sum_send.at[1])
        all_of(sums_z.at[0:n_row - 1, 0:2], sum_send.at[0])
        all_of(bank.at[0:31], bank_send.at[0])

        @pl.when(is_home)
        def _():
            for c in help_copies:
                c().wait_send()
            remote(pts, rows.at[slots - 1], pts_send.at[0], pts_recv.at[slots - 1], partner).wait_recv()

        @pl.when(is_helper)
        def _():
            for c in back_copies:
                c().wait_send()
        y_copy.wait()
        c_copy.wait()

    phase_enter()
    phase_setup()
    order = smooth[0]
    root = jnp.where(order >= 2, math.sqrt(5.0), jnp.where(order >= 1, math.sqrt(3.0), 1.0)).astype(F32)
    scale = (root * LOG2E) / jnp.full((8, LANES), reach[0], F32)
    linear = jnp.where(order >= 1, 1.0 / LOG2E, 0.0).astype(F32)
    square = jnp.where(order >= 2, 1.0 / (3.0 * LOG2E * LOG2E), 0.0).astype(F32)
    phase_barrier()
    phase_points()
    step_near()
    phase_clear()
    step_own()
    phase_rows(0)
    tile(0, 0, 1)
    step_first(1)
    step_first(3)
    tile(0, 1, 2)
    phase_rows(1)
    phase_rows(2)
    step_first(2)
    tile(0, 2, 4)
    step_second(0)
    tile(0, 4, 8)
    tile(1, 0, 2)
    step_second(1)
    tile(1, 2, 4)
    step_second(3)
    tile(1, 4, 8)
    phase_cols()
    tile(2, 0, 2)
    step_half(0)
    step_second(2)
    tile(2, 2, 4)
    step_half(1)
    tile(2, 4, 6)
    step_half(3)
    tile(2, 6, 8)
    phase_share()
    send_z()
    wait_bank()
    phase_project()
    wait_z()
    send_p()
    phase_solve()
    phase_far_y()
    phase_far()
    total_error()
    wait_sends()


def solution(mesh):
    n_row, n_col = mesh.shape["prow"], mesh.shape["pcol"]

    def per_device(points, range_length, smoothness, sketch_bank, sketch_ids, tile_ranks):
        slots = sketch_ids.shape[0]
        nb = points.shape[3]
        rmax = sketch_bank.shape[1]
        dims = (slots, n_row, n_col, nb, rmax)
        anywhere = pl.BlockSpec(memory_space=pl.ANY)
        vmem = pltpu.VMEM
        hbm = pl.BlockSpec(memory_space=pltpu.HBM)
        scalars = pl.BlockSpec(memory_space=pltpu.SMEM)
        smem = pltpu.SMEM
        dma = pltpu.SemaphoreType.DMA
        y_out, c_out, err, rank = pl.pallas_call(
            functools.partial(kernel, dims),
            out_shape=(
                jax.ShapeDtypeStruct((slots, rmax, nb), F32),
                jax.ShapeDtypeStruct((slots, rmax, nb), F32),
                jax.ShapeDtypeStruct((slots,), F32),
                jax.ShapeDtypeStruct((1,), jnp.int32),
            ),
            in_specs=[hbm] * 6,
            out_specs=(anywhere, anywhere, scalars, scalars),
            scratch_shapes=[
                smem((1,), F32), smem((1,), jnp.int32), smem((slots,), jnp.int32), smem((slots,), jnp.int32),
                vmem((2, nb), F32), vmem((slots, 2, nb), F32), vmem((2, nb), F32),
                vmem((n_col, rmax, nb), BF16), vmem((3, nb, nb), BF16),
                vmem((3, 2, nb, LANES), F32), vmem((8, nb), F32), vmem((8, nb), F32),
                vmem((3, 3 * rmax, nb), BF16), vmem((4, rmax, nb), F32), vmem((3, rmax, nb), F32),
                vmem((4, rmax, nb), F32), vmem((3, rmax, nb), F32), vmem((2, 3, rmax, rmax), F32),
                vmem((3, 8, LANES), F32), vmem((3, 8, LANES), F32),
                vmem((8, LANES), jnp.int32), vmem((8, LANES), jnp.int32),
                vmem((rmax, nb), BF16), vmem((rmax, nb), BF16), vmem((rmax, nb), BF16), vmem((rmax, nb), BF16),
                vmem((8, LANES), F32), vmem((n_row, 8, LANES), F32), vmem((n_col, 8, LANES), F32),
                dma((6,)), dma((3,)), dma((8,)), dma((slots,)), dma((5,)), dma((5,)),
                dma((1,)), dma((4,)), dma((4,)), dma((4,)), dma((1,)), dma((2,)), dma((2,)), dma((2,)),
            ],
            compiler_params=pltpu.CompilerParams(
                collective_id=0, has_side_effects=True, vmem_limit_bytes=VMEM_BYTES),
        )(
            *(pltpu.with_memory_space_constraint(v, pltpu.HBM) for v in (
                points.reshape(2, nb), sketch_bank.reshape(rmax, nb),
                sketch_ids.reshape(slots), tile_ranks.reshape(slots))), range_length, smoothness,
        )
        return (
            y_out.reshape(slots, 1, 1, 1, rmax, nb),
            c_out.reshape(slots, 1, 1, 1, rmax, nb),
            err.reshape(slots, 1, 1, 1),
            rank,
        )

    return jax.shard_map(
        per_device,
        mesh=mesh,
        in_specs=(
            P(None, "pcol", None, None),
            P(),
            P(),
            P("pcol", None, None),
            P(None, "prow", None, "pcol"),
            P(None, "prow", None, "pcol"),
        ),
        out_specs=(
            P(None, "prow", None, "pcol", None, None),
            P(None, "prow", None, "pcol", None, None),
            P(None, "prow", None, "pcol"),
            P(),
        ),
        check_vma=False,
    )
```
